128 devices in a mesh: row: 8 (over z, y_hi), col: 16 (over y_lo, x, core).
Axes of the slice: x: 4, y: 4 (y_hi: 2, y_lo: 2; y = y_hi * 2 + y_lo), z: 4, core: 2. Of those that a mesh axis runs over, the one named last changes fastest.
Arguments:
- matrix_tiles: float32 [8, 16, 16, 512, 512], P('row', 'col'), may hold values from -0.25 to 0.25
- tile_rows: int32 [8, 16, 16], P('row', 'col'), may hold values from 0 to 127, as said below
- tile_columns: int32 [8, 16, 16], P('row', 'col'), may hold values from 0 to 63, as said below
- tile_counts: int32 [8, 16], P('row', 'col'), may hold values from 8 to 16, as said below
- primal_iter: float32 [2, 524288], P(None, ('col', 'row')), may hold values from -6 to 6
- dual_iter: float32 [2, 524288], P(None, ('row', 'col')), may hold values from -6 to 6
- requirement: float32 [524288], P('row'), may hold values from -68 to 68
- constraint_kind: int32 [524288], P('row'), may hold values from 0 to 1
- objective: float32 [524288], P('col'), may hold values from -68 to 68
- lower_bound: float32 [524288], P('col'), may hold values from -1.5 to 1.5
- upper_bound: float32 [524288], P('col'), may hold values from -1.5 to 1.5
- variable_kind: int32 [524288], P('col'), may hold values from 0 to 3
Outputs:
- primal_residual: float32 [2, 524288], P(None, ('row', 'col'))
- dual_residual: float32 [2, 524288], P(None, ('col', 'row'))
- metrics: float32 [2, 3], replicated
The draws below stay inside these ranges and needn't reach their ends.
Inputs may be any that keep to these rules, and one draw needn't show every extreme that they name: `tile_counts`: slots below the count of a list hold live tiles, the others are padding; some list has all 16 slots live. `tile_rows`: in each constraint group, the first (8) slots of its lists name every block row of the group exactly once; later slots name any block row, and repeated tiles add. `tile_columns`: in each variable group, the first (8) slots of its lists name every block column of the group exactly once; later slots name any block column, and repeated tiles add. `constraint_kind`: 0 marks an equality, 1 a constraint of the form at least. `variable_kind`: 0 free, 1 lower bound only, 2 upper bound only, 3 both bounds.
All inputs are finite; a program needn't handle non-finite values.
Results may differ from the reference program's by a relative error of at most 0.0003.
Values sent between devices are 32-bit elements; how exact they have to be, the bound alone decides.
A program may use at most 64 MiB of HBM per device.

```python
import math
import jax
import jax.numpy as jnp
from jax import lax

BLK = 512
TILES_DEV = 16
CANDS = 2
RBG = 128
CBG = 64
NROW = 524288
NCOL = 524288
N_ROW = 8
N_COL = 16


def rising_vector(key, length):
    first_key, second_key = jax.random.split(key)
    position = jnp.arange(length, dtype=jnp.float32) / length
    values = jnp.clip(jax.random.normal(first_key, (length,), jnp.float32), -5.0, 5.0)
    growth = jnp.exp(position * math.log(3.0))
    spread = jnp.exp(jax.random.uniform(second_key, (length,), jnp.float32, 0.0, math.log(10.0)))
    return (0.15 * values * spread * growth).astype(jnp.float32)


def draw_requirement(key, part):
    return rising_vector(jax.random.fold_in(key, 11), NROW)


def draw_objective(key, part):
    return rising_vector(jax.random.fold_in(key, 12), NCOL)


def draw_tile_counts(key, part):
    first_key, second_key = jax.random.split(jax.random.fold_in(key, 13))
    counts = jax.random.randint(first_key, (N_ROW * N_COL,), TILES_DEV // 2, TILES_DEV + 1)
    chosen = jax.random.randint(second_key, (), 0, N_ROW * N_COL)
    flattened = jnp.where(jnp.arange(N_ROW * N_COL) == chosen, TILES_DEV, counts)
    return flattened.reshape(N_ROW, N_COL).astype(jnp.int32)


def draw_tile_rows(key, part):
    half = TILES_DEV // 2
    perm_keys = jax.random.split(jax.random.fold_in(key, 21), N_ROW)
    covering = jax.vmap(lambda single: jax.random.permutation(single, RBG))(perm_keys)
    covering = covering.reshape(N_ROW, N_COL, half)
    extra = jax.random.randint(jax.random.fold_in(key, 22), (N_ROW, N_COL, TILES_DEV - half), 0, RBG)
    return jnp.concatenate([covering.astype(jnp.int32), extra.astype(jnp.int32)], axis=2)


def draw_tile_columns(key, part):
    half = TILES_DEV // 2
    perm_keys = jax.random.split(jax.random.fold_in(key, 31), N_COL)
    covering = jax.vmap(lambda single: jax.random.permutation(single, CBG))(perm_keys)
    covering = jnp.transpose(covering.reshape(N_COL, N_ROW, half), (1, 0, 2))
    extra = jax.random.randint(jax.random.fold_in(key, 32), (N_ROW, N_COL, TILES_DEV - half), 0, CBG)
    return jnp.concatenate([covering.astype(jnp.int32), extra.astype(jnp.int32)], axis=2)


def touch_ends(entries, rng, smallest, high):
    longest = entries.shape.index(max(entries.shape))
    spots = []
    for shift in (0, 1):
        where = [jax.random.randint(jax.random.fold_in(rng, axis), (), 0, length) for axis, length in enumerate(entries.shape)]
        where[longest] = (where[longest] + shift) % entries.shape[longest]
        spots.append(tuple(where))
    return entries.at[spots[0]].set(smallest).at[spots[1]].set(high)


def level_of(own_key, extent, cuts, low, largest):
    def one(dim, parts):
        heights = jax.random.uniform(jax.random.fold_in(jax.random.fold_in(own_key, 6), dim), (parts,), jnp.float32, low / len(cuts), largest / len(cuts))
        return jnp.repeat(jnp.exp(heights), extent[dim] // parts).reshape((-1,) + (1,) * (len(extent) - dim - 1))

    gain = one(*cuts[0])
    for cut in cuts[1:]:
        gain = gain * one(*cut)
    return gain


def gaussian(stream_key, shape, scale, limit, shards=(), kind=jnp.bfloat16):
    factor_of = level_of(stream_key, shape, shards, -0.22, 0.18) if shards else 1.0
    entries = jax.random.normal(stream_key, shape, jnp.float32) * scale * factor_of
    return jnp.minimum(jnp.maximum(entries, -limit), limit).astype(kind)


def setup_inputs(seed: int = 0) -> dict:
    keys = jax.random.split(jax.random.key(seed), 13)
    return {
        "matrix_tiles": gaussian(keys[0], (N_ROW, N_COL, TILES_DEV, BLK, BLK), BLK ** -0.5, 0.25, ((0, 8), (1, 16)), jnp.float32),
        "tile_rows": draw_tile_rows(jax.random.fold_in(keys[12], 71), 0),
        "tile_columns": draw_tile_columns(jax.random.fold_in(keys[12], 71), 0),
        "tile_counts": draw_tile_counts(jax.random.fold_in(keys[12], 71), 0),
        "primal_iter": gaussian(keys[4], (CANDS, NCOL), 1.0, 6.0, ((1, 128),), jnp.float32),
        "dual_iter": gaussian(keys[5], (CANDS, NROW), 1.0, 6.0, ((1, 128),), jnp.float32),
        "requirement": draw_requirement(jax.random.fold_in(keys[12], 71), 0),
        "constraint_kind": touch_ends(jax.random.randint(keys[7], (NROW,), 0, 2), jax.random.fold_in(keys[7], 1), 0, 1).astype(jnp.int32),
        "objective": draw_objective(jax.random.fold_in(keys[12], 71), 0),
        "lower_bound": jnp.clip(jax.random.uniform(keys[9], (NCOL,), jnp.float32, -1.5, 1.5) * level_of(keys[9], (NCOL,), ((0, 16),), -0.4, 0.0), -1.5, 1.5),
        "upper_bound": jnp.clip(jax.random.uniform(keys[10], (NCOL,), jnp.float32, -1.5, 1.5) * level_of(keys[10], (NCOL,), ((0, 16),), -0.4, 0.0), -1.5, 1.5),
        "variable_kind": touch_ends(jax.random.randint(keys[11], (NCOL,), 0, 4), jax.random.fold_in(keys[11], 1), 0, 3).astype(jnp.int32),
    }


HIGHEST_PRECISION = lax.Precision.HIGHEST

def primal_side(product, require_part, kind_part, dual_part):
    difference = require_part[None, :] - product
    residual = jnp.where(kind_part[None, :] == 1, jnp.maximum(difference, 0.0), difference)
    return (residual, lax.optimization_barrier(jnp.sum(residual * residual, axis=1)), jnp.sum(require_part * require_part), lax.optimization_barrier(jnp.sum(require_part[None, :] * dual_part, axis=1)))

def dual_side(transposed, objective, lower_bound, upper_bound, variable_kind, primal_part):
    reduced = objective[None, :] - transposed
    lower_active = (variable_kind == 1) | (variable_kind == 3)
    upper_active = (variable_kind == 2) | (variable_kind == 3)
    multiplier = jnp.where(lower_active[None, :], jnp.maximum(reduced, 0.0), 0.0) + jnp.where(upper_active[None, :], jnp.minimum(reduced, 0.0), 0.0)
    residual = reduced - multiplier
    bound_sum = lax.optimization_barrier(jnp.sum(lower_bound[None, :] * jnp.maximum(multiplier, 0.0) + upper_bound[None, :] * jnp.minimum(multiplier, 0.0), axis=1))
    return (residual, lax.optimization_barrier(jnp.sum(residual * residual, axis=1)), jnp.sum(objective * objective), lax.optimization_barrier(jnp.sum(objective[None, :] * primal_part, axis=1)), bound_sum)

def finish(primal_square, require_square, require_dot, dual_square, objective_square, objective_dot, bound_sum):
    primal_ratio = jnp.sqrt(primal_square) / (1.0 + jnp.sqrt(require_square))
    dual_ratio = jnp.sqrt(dual_square) / (1.0 + jnp.sqrt(objective_square))
    dual_value = require_dot + bound_sum
    duality_gap = jnp.abs(objective_dot - dual_value) / (1.0 + jnp.abs(objective_dot) + jnp.abs(dual_value))
    return jnp.stack([primal_ratio, dual_ratio, duality_gap], axis=1)

def reference(matrix_tiles, tile_rows, tile_columns, tile_counts, primal_iter, dual_iter, requirement, constraint_kind, objective, lower_bound, upper_bound, variable_kind):
    block_size = matrix_tiles.shape[-1]
    slot_count = matrix_tiles.shape[2]
    groups = N_ROW * N_COL
    row_blocks = requirement.shape[0] // block_size // N_ROW
    column_blocks = objective.shape[0] // block_size // N_COL
    candidates = primal_iter.shape[0]
    primal_blocks = primal_iter.reshape(candidates, -1, block_size)
    dual_blocks = dual_iter.reshape(candidates, -1, block_size)
    flat_tiles = matrix_tiles.reshape(groups, slot_count, block_size, block_size)

    def accumulate(totals, inputs):
        product, transposed = totals
        own_tiles, rows_here, columns_here, count_here, device_index = inputs
        global_rows = device_index // N_COL * row_blocks + rows_here
        global_columns = device_index % N_COL * column_blocks + columns_here
        active = (lax.iota(jnp.int32, slot_count) < count_here).astype(own_tiles.dtype)
        primal_pick = primal_blocks[:, global_columns, :] * active[None, :, None]
        dual_pick = dual_blocks[:, global_rows, :] * active[None, :, None]
        tile_product = jnp.einsum('tij,stj->sti', own_tiles, primal_pick, precision=HIGHEST_PRECISION)
        tile_transposed = jnp.einsum('tij,sti->stj', own_tiles, dual_pick, precision=HIGHEST_PRECISION)
        product = product.at[:, global_rows, :].add(tile_product)
        transposed = transposed.at[:, global_columns, :].add(tile_transposed)
        return ((product, transposed), None)
    start = (jnp.zeros(dual_blocks.shape, matrix_tiles.dtype), jnp.zeros(primal_blocks.shape, matrix_tiles.dtype))
    inputs = (flat_tiles, tile_rows.reshape(groups, slot_count), tile_columns.reshape(groups, slot_count), tile_counts.reshape(groups), jnp.arange(groups, dtype=jnp.int32))
    (product, transposed), _ = lax.scan(accumulate, start, inputs)
    product = product.reshape(candidates, -1)
    transposed = transposed.reshape(candidates, -1)
    primal_residual, primal_square, require_square, require_dot = primal_side(product, requirement, constraint_kind, dual_iter)
    dual_residual, dual_square, objective_square, objective_dot, bound_sum = dual_side(transposed, objective, lower_bound, upper_bound, variable_kind, primal_iter)
    metrics = finish(primal_square, require_square, require_dot, dual_square, objective_square, objective_dot, bound_sum)
    return (primal_residual, dual_residual, metrics)
```

```python
import functools

import jax
import jax.numpy as jnp
from jax import lax
from jax.experimental import pallas as pl
from jax.experimental.pallas import tpu as pltpu
from jax.sharding import Mesh
from jax.sharding import PartitionSpec as P

ROW = ("row_0", "row_1")
COL = ("col_0", "col_1", "col_2")
ROW_COL = ROW + COL
COL_ROW = COL + ROW
MESH_ID = pl.DeviceIdType.MESH

BLK = 512
SLOTS = 16
ROW_BLOCKS = 128
COL_BLOCKS = 64
OWN = 64

ROW_OFFS = [(dz, dy) for dz in range(4) for dy in range(2)]
COL_OFFS = [(dy, dx, dc) for dy in range(2) for dx in range(4) for dc in range(2)]
F32 = jnp.float32
BF16 = jnp.bfloat16


def split2(v):
    hi = v.astype(BF16)
    lo = (v - hi.astype(F32)).astype(BF16)
    return hi, lo


def spread(v):
    sub = lax.broadcasted_iota(jnp.int32, (8, 128), 0)
    hi = v.astype(BF16).astype(F32)
    lo = v - hi
    parts = []
    for k in range(4):
        keep = (sub // 2) == k
        parts.append(jnp.concatenate([jnp.where(keep, hi, 0.0), jnp.where(keep, lo, 0.0)], axis=0))
    return jnp.concatenate(parts, axis=1).astype(BF16)


def gathered(r):
    sub = lax.broadcasted_iota(jnp.int32, (8, 128), 0)
    out = jnp.zeros((8, 128), F32)
    for g in range(4):
        c = r[:8, 128 * g : 128 * g + 128] + r[8:, 128 * g : 128 * g + 128]
        c = c + pltpu.roll(c, 2, 0)
        c = c + pltpu.roll(c, 4, 0)
        out = jnp.where((sub // 2) == g, c, out)
    return out


def kernel(
    rows_ref,
    cols_ref,
    count_ref,
    tiles_ref,
    primal_ref,
    dual_ref,
    req_ref,
    ckind_ref,
    obj_ref,
    low_ref,
    up_ref,
    vkind_ref,
    pres_ref,
    dres_ref,
    met_ref,
    tiles,
    a_hi,
    a_lo,
    xg,
    yg,
    xo,
    yo,
    pbuf,
    part,
    tpart,
    precv,
    trecv,
    small,
    ismall,
    col_stat,
    row_stat,
    tile_sem,
    in_sem,
    row_send,
    row_recv,
    col_send,
    col_recv,
    prs_send,
    prs_recv,
    trs_send,
    trs_recv,
    cst_send,
    cst_recv,
    rst_send,
    rst_recv,
):
    z = lax.axis_index("row_0")
    yh = lax.axis_index("row_1")
    yl = lax.axis_index("col_0")
    x = lax.axis_index("col_1")
    core = lax.axis_index("col_2")
    r_me = z * 2 + yh
    c_me = (yl * 4 + x) * 2 + core

    def row_peer(off):
        pz, py = lax.rem(z + off[0], 4), lax.rem(yh + off[1], 2)
        return (pz, py, yl, x, core), pz * 2 + py

    def col_peer(off):
        py, px, pc = lax.rem(yl + off[0], 2), lax.rem(x + off[1], 4), lax.rem(core + off[2], 2)
        return (z, yh, py, px, pc), (py * 4 + px) * 2 + pc

    barrier = pltpu.get_barrier_semaphore()
    for off in ROW_OFFS[1:]:
        pl.semaphore_signal(barrier, inc=1, device_id=row_peer(off)[0], device_id_type=MESH_ID)
    for off in COL_OFFS[1:]:
        pl.semaphore_signal(barrier, inc=1, device_id=col_peer(off)[0], device_id_type=MESH_ID)

    own_x = pl.ds(r_me * 8, 8)
    own_y = pl.ds(c_me * 8, 8)
    cp_x = pltpu.make_async_copy(primal_ref.reshape(8, 8, 128), xg.at[own_x], in_sem.at[0])
    cp_y = pltpu.make_async_copy(dual_ref.reshape(8, 8, 128), yg.at[own_y], in_sem.at[1])
    cp_x.start()
    cp_y.start()
    own_copies = [
        pltpu.make_async_copy(primal_ref, xo, in_sem.at[8]),
        pltpu.make_async_copy(dual_ref, yo, in_sem.at[9]),
    ]
    mine_r = pl.ds(pl.multiple_of(c_me * 32, 32), 32)
    mine_c = pl.ds(pl.multiple_of(r_me * 32, 32), 32)
    extra = own_copies + [
        pltpu.make_async_copy(req_ref.at[mine_r], small.at[0], in_sem.at[2]),
        pltpu.make_async_copy(obj_ref.at[mine_c], small.at[1], in_sem.at[3]),
        pltpu.make_async_copy(low_ref.at[mine_c], small.at[2], in_sem.at[4]),
        pltpu.make_async_copy(up_ref.at[mine_c], small.at[3], in_sem.at[5]),
        pltpu.make_async_copy(ckind_ref.at[mine_r], ismall.at[0], in_sem.at[6]),
        pltpu.make_async_copy(vkind_ref.at[mine_c], ismall.at[1], in_sem.at[7]),
    ]
    for cp in extra:
        cp.start()

    def tile_copy(t):
        return pltpu.make_async_copy(tiles_ref.at[t], tiles.at[t], tile_sem.at[t])

    for t in range(SLOTS):
        tile_copy(t).start()

    cp_x.wait()
    cp_y.wait()
    pl.semaphore_wait(barrier, len(ROW_OFFS) + len(COL_OFFS) - 2)

    row_gather = []
    for i, off in enumerate(ROW_OFFS[1:]):
        row_gather.append(
            pltpu.make_async_remote_copy(
                src_ref=xg.at[own_x],
                dst_ref=xg.at[own_x],
                send_sem=row_send.at[i],
                recv_sem=row_recv.at[i],
                device_id=row_peer(off)[0],
                device_id_type=MESH_ID,
            )
        )
    col_gather = []
    for i, off in enumerate(COL_OFFS[1:]):
        col_gather.append(
            pltpu.make_async_remote_copy(
                src_ref=yg.at[own_y],
                dst_ref=yg.at[own_y],
                send_sem=col_send.at[i],
                recv_sem=col_recv.at[i],
                device_id=col_peer(off)[0],
                device_id_type=MESH_ID,
            )
        )
    for cp in row_gather:
        cp.start()
    for cp in col_gather:
        cp.start()

    lane = lax.broadcasted_iota(jnp.int32, (8, 128), 1)
    count = count_ref[0, 0]
    ridx = jnp.full((8, 128), -1, jnp.int32)
    cidx = jnp.full((8, 128), -1, jnp.int32)
    for t in range(SLOTS):
        here = (lax.rem(lane, SLOTS) == t) & (lane < 3 * SLOTS) & (jnp.full((8, 128), t, jnp.int32) < count)
        ridx = jnp.where(here, rows_ref[0, t], ridx)
        cidx = jnp.where(here, cols_ref[0, t], cidx)
    r_iota = lax.broadcasted_iota(jnp.int32, (ROW_BLOCKS, 128), 0)
    c_iota = lax.broadcasted_iota(jnp.int32, (COL_BLOCKS, 128), 0)
    r_hot = jnp.where(r_iota == ridx[:1], 1.0, 0.0).astype(BF16)[:, : 3 * SLOTS]
    c_hot = jnp.where(c_iota == cidx[:1], 1.0, 0.0).astype(BF16)[:, : 3 * SLOTS]

    def convert(t, carry):
        tile_copy(t).wait()

        def piece(i, c):
            sl = pl.ds(pl.multiple_of(i * 64, 64), 64)
            hi, lo = split2(tiles[t, sl, :])
            a_hi[t, sl, :] = hi
            a_lo[t, sl, :] = lo
            return c

        return lax.fori_loop(0, BLK // 64, piece, carry, unroll=True)

    lax.fori_loop(0, SLOTS, convert, 0)

    def scatter(hot, dest, blocks):
        cols = []
        for e in range(8):
            v = pbuf[pl.ds(e, SLOTS, stride=8), :]
            hi = v.astype(BF16)
            rest = v - hi.astype(F32)
            mid = rest.astype(BF16)
            lo = (rest - mid.astype(F32)).astype(BF16)
            cols.append(jnp.concatenate([hi, mid, lo], axis=0))
        rhs = jnp.concatenate(cols, axis=1)
        out = jnp.dot(hot, rhs, preferred_element_type=F32)
        for e in range(8):
            dest[pl.ds(e, blocks, stride=8), :] = out[:, e * 128 : (e + 1) * 128]

    for cp in row_gather:
        cp.wait_recv()

    def forward(t, carry):
        lhs = spread(xg[cols_ref[0, t]])
        dims = (((1,), (1,)), ((), ()))
        res = lax.dot_general(lhs, a_hi[t], dims, preferred_element_type=F32)
        res = res + lax.dot_general(lhs, a_lo[t], dims, preferred_element_type=F32)
        pbuf[pl.ds(pl.multiple_of(t * 8, 8), 8), :] = gathered(res)
        return carry

    lax.fori_loop(0, SLOTS, forward, 0)
    scatter(r_hot, part, ROW_BLOCKS)

    prs = []
    for i, off in enumerate(COL_OFFS[1:]):
        dev, idx = col_peer(off)
        prs.append(
            pltpu.make_async_remote_copy(
                src_ref=part.at[pl.ds(pl.multiple_of(idx * OWN, OWN), OWN)],
                dst_ref=precv.at[i],
                send_sem=prs_send.at[i],
                recv_sem=prs_recv.at[i],
                device_id=dev,
                device_id_type=MESH_ID,
            )
        )
    for cp in prs:
        cp.start()

    for cp in col_gather:
        cp.wait_recv()

    def backward(t, carry):
        lhs = spread(yg[rows_ref[0, t]])
        res = jnp.dot(lhs, a_hi[t], preferred_element_type=F32)
        res = res + jnp.dot(lhs, a_lo[t], preferred_element_type=F32)
        pbuf[pl.ds(pl.multiple_of(t * 8, 8), 8), :] = gathered(res)
        return carry

    lax.fori_loop(0, SLOTS, backward, 0)
    scatter(c_hot, tpart, COL_BLOCKS)

    trs = []
    for i, off in enumerate(ROW_OFFS[1:]):
        dev, idx = row_peer(off)
        trs.append(
            pltpu.make_async_remote_copy(
                src_ref=tpart.at[pl.ds(pl.multiple_of(idx * OWN, OWN), OWN)],
                dst_ref=trecv.at[i],
                send_sem=trs_send.at[i],
                recv_sem=trs_recv.at[i],
                device_id=dev,
                device_id_type=MESH_ID,
            )
        )
    for cp in trs:
        cp.start()

    for cp in extra:
        cp.wait()
    for cp in prs:
        cp.wait_recv()
    product = part[pl.ds(pl.multiple_of(c_me * OWN, OWN), OWN), :]
    for i in range(len(prs)):
        product = product + precv[i]
    pres_ref[...] = product
    sums = []
    req = small[0]
    is_ge = ismall[0] == 1
    dual_own = [yo[pl.ds(s, 32, stride=2), :] for s in range(2)]
    primal_own = [xo[pl.ds(s, 32, stride=2), :] for s in range(2)]
    stat_rows = [[], []]

    def total(v):
        return jnp.sum(v.reshape(4, 8, 128), axis=0)

    for s in range(2):
        diff = req - pres_ref[pl.ds(s, 32, stride=2), :]
        res = jnp.where(is_ge, jnp.maximum(diff, 0.0), diff)
        pres_ref[pl.ds(s, 32, stride=2), :] = res
        stat_rows[s] += [total(res * res), total(req * req), total(req * dual_own[s])]

    for cp in trs:
        cp.wait_recv()
    transposed = tpart[pl.ds(pl.multiple_of(r_me * OWN, OWN), OWN), :]
    for i in range(len(trs)):
        transposed = transposed + trecv[i]
    dres_ref[...] = transposed
    obj, low, up, vk = small[1], small[2], small[3], ismall[1]
    low_on = (vk == 1) | (vk == 3)
    up_on = (vk == 2) | (vk == 3)
    for s in range(2):
        reduced = obj - dres_ref[pl.ds(s, 32, stride=2), :]
        mult = jnp.where(low_on, jnp.maximum(reduced, 0.0), 0.0) + jnp.where(
            up_on, jnp.minimum(reduced, 0.0), 0.0
        )
        res = reduced - mult
        dres_ref[pl.ds(s, 32, stride=2), :] = res
        bound = low * jnp.maximum(mult, 0.0) + up * jnp.minimum(mult, 0.0)
        stat_rows[s] += [
            total(res * res),
            total(obj * obj),
            total(obj * primal_own[s]),
            total(bound),
        ]
    lane1 = lax.broadcasted_iota(jnp.int32, (1, 128), 1)
    for s in range(2):
        acc = jnp.zeros((1, 128), F32)
        for q in range(7):
            v = jnp.sum(stat_rows[s][q], axis=0, keepdims=True)
            v = jnp.sum(v, axis=1, keepdims=True)
            acc = jnp.where(lane1 == q, v, acc)
        col_stat[c_me, pl.ds(s, 1), :] = acc

    cst = []
    for i, off in enumerate(COL_OFFS[1:]):
        cst.append(
            pltpu.make_async_remote_copy(
                src_ref=col_stat.at[c_me],
                dst_ref=col_stat.at[c_me],
                send_sem=cst_send.at[i],
                recv_sem=cst_recv.at[i],
                device_id=col_peer(off)[0],
                device_id_type=MESH_ID,
            )
        )
    for cp in cst:
        cp.start()
    for cp in cst:
        cp.wait_recv()
    row_stat[r_me] = jnp.sum(col_stat[...], axis=0)
    rst = []
    for i, off in enumerate(ROW_OFFS[1:]):
        rst.append(
            pltpu.make_async_remote_copy(
                src_ref=row_stat.at[r_me],
                dst_ref=row_stat.at[r_me],
                send_sem=rst_send.at[i],
                recv_sem=rst_recv.at[i],
                device_id=row_peer(off)[0],
                device_id_type=MESH_ID,
            )
        )
    for cp in rst:
        cp.start()
    for cp in rst:
        cp.wait_recv()
    acc = jnp.sum(row_stat[...], axis=0)

    pick = [acc[:, q : q + 1] for q in range(7)]
    primal_square, require_square, require_dot = pick[0], pick[1], pick[2]
    dual_square, objective_square, objective_dot, bound_sum = pick[3], pick[4], pick[5], pick[6]
    primal_ratio = jnp.sqrt(primal_square) / (1.0 + jnp.sqrt(require_square))
    dual_ratio = jnp.sqrt(dual_square) / (1.0 + jnp.sqrt(objective_square))
    dual_value = require_dot + bound_sum
    gap = jnp.abs(objective_dot - dual_value) / (1.0 + jnp.abs(objective_dot) + jnp.abs(dual_value))
    lane2 = lax.broadcasted_iota(jnp.int32, (2, 128), 1)
    met = jnp.where(lane2 == 0, primal_ratio, jnp.where(lane2 == 1, dual_ratio, gap))
    met_ref[...] = met[:, :3]

    for group in (row_gather, col_gather, prs, trs, cst, rst):
        for cp in group:
            cp.wait_send()


def interleave(a):
    return a.reshape(2, 32, 128).transpose(1, 0, 2).reshape(OWN, 128)


def deinterleave(a):
    return a.reshape(32, 2, 128).transpose(1, 0, 2).reshape(2, 4096)


def on_device(
    matrix_tiles,
    tile_rows,
    tile_columns,
    tile_counts,
    primal_iter,
    dual_iter,
    requirement,
    constraint_kind,
    objective,
    lower_bound,
    upper_bound,
    variable_kind,
):
    hbm = pl.BlockSpec(memory_space=pl.ANY)
    smem = pl.BlockSpec(memory_space=pltpu.SMEM)
    vmem = pl.BlockSpec(memory_space=pltpu.VMEM)
    n_row, n_col = len(ROW_OFFS) - 1, len(COL_OFFS) - 1
    dma = pltpu.SemaphoreType.DMA
    pres, dres, metrics = pl.pallas_call(
        kernel,
        name="restart_check",
        out_shape=(
            jax.ShapeDtypeStruct((OWN, 128), F32),
            jax.ShapeDtypeStruct((OWN, 128), F32),
            jax.ShapeDtypeStruct((2, 3), F32),
        ),
        in_specs=[smem] * 3 + [hbm] * 9,
        out_specs=(vmem, vmem, vmem),
        scratch_shapes=[
            pltpu.VMEM((SLOTS, BLK, BLK), F32),
            pltpu.VMEM((SLOTS, BLK, BLK), BF16),
            pltpu.VMEM((SLOTS, BLK, BLK), BF16),
            pltpu.VMEM((COL_BLOCKS, 8, 128), F32),
            pltpu.VMEM((ROW_BLOCKS, 8, 128), F32),
            pltpu.VMEM((OWN, 128), F32),
            pltpu.VMEM((OWN, 128), F32),
            pltpu.VMEM((SLOTS * 8, 128), F32),
            pltpu.VMEM((16 * OWN, 128), F32),
            pltpu.VMEM((8 * OWN, 128), F32),
            pltpu.VMEM((n_col, OWN, 128), F32),
            pltpu.VMEM((n_row, OWN, 128), F32),
            pltpu.VMEM((4, 32, 128), F32),
            pltpu.VMEM((2, 32, 128), jnp.int32),
            pltpu.VMEM((n_col + 1, 2, 128), F32),
            pltpu.VMEM((n_row + 1, 2, 128), F32),
            dma((SLOTS,)),
            dma((10,)),
            dma((n_row,)),
            dma((n_row,)),
            dma((n_col,)),
            dma((n_col,)),
            dma((n_col,)),
            dma((n_col,)),
            dma((n_row,)),
            dma((n_row,)),
            dma((n_col,)),
            dma((n_col,)),
            dma((n_row,)),
            dma((n_row,)),
        ],
        compiler_params=pltpu.CompilerParams(
            collective_id=0, has_side_effects=True, vmem_limit_bytes=60 * 1024 * 1024
        ),
    )(
        tile_rows.reshape(1, SLOTS),
        tile_columns.reshape(1, SLOTS),
        tile_counts,
        matrix_tiles.reshape(SLOTS, BLK, BLK),
        interleave(primal_iter),
        interleave(dual_iter),
        requirement.reshape(512, 128),
        constraint_kind.reshape(512, 128),
        objective.reshape(256, 128),
        lower_bound.reshape(256, 128),
        upper_bound.reshape(256, 128),
        variable_kind.reshape(256, 128),
    )
    return deinterleave(pres), deinterleave(dres), metrics


def solution(mesh):
    torus = Mesh(mesh.devices.reshape(4, 2, 2, 4, 2), ROW_COL)
    return jax.shard_map(
        on_device,
        mesh=torus,
        in_specs=(
            P(ROW, COL, None, None, None),
            P(ROW, COL, None),
            P(ROW, COL, None),
            P(ROW, COL),
            P(None, COL_ROW),
            P(None, ROW_COL),
            P(ROW),
            P(ROW),
            P(COL),
            P(COL),
            P(COL),
            P(COL),
        ),
        out_specs=(P(None, ROW_COL), P(None, COL_ROW), P()),
        check_vma=False,
    )
```

```python
import jax
import jax.numpy as jnp
from jax import lax
from jax.experimental import pallas as pl
from jax.experimental.pallas import tpu as pltpu
from jax.sharding import Mesh
from jax.sharding import PartitionSpec as P

ROW = ("row_0", "row_1")
COL = ("col_0", "col_1", "col_2")
ROW_COL = ROW + COL
COL_ROW = COL + ROW
MESH_ID = pl.DeviceIdType.MESH

BLK = 512
SLOTS = 16
ROW_BLOCKS = 128
COL_BLOCKS = 64
OWN = 64

CHIP_OFFS = [(1, 2), (1, 1), (1, 3), (0, 2), (1, 0), (0, 1), (0, 3), (0, 0)]
F32 = jnp.float32
BF16 = jnp.bfloat16


def split2(v):
    hi = v.astype(BF16)
    lo = (v - hi.astype(F32)).astype(BF16)
    return hi, lo


def spread(v):
    sub = lax.broadcasted_iota(jnp.int32, (8, 128), 0)
    hi = v.astype(BF16).astype(F32)
    lo = v - hi
    parts = []
    for k in range(4):
        keep = (sub // 2) == k
        parts.append(jnp.concatenate([jnp.where(keep, hi, 0.0), jnp.where(keep, lo, 0.0)], axis=0))
    return jnp.concatenate(parts, axis=1).astype(BF16)


def gathered(r):
    sub = lax.broadcasted_iota(jnp.int32, (8, 128), 0)
    out = jnp.zeros((8, 128), F32)
    for g in range(4):
        c = r[:8, 128 * g : 128 * g + 128] + r[8:, 128 * g : 128 * g + 128]
        c = c + pltpu.roll(c, 2, 0)
        c = c + pltpu.roll(c, 4, 0)
        out = jnp.where((sub // 2) == g, c, out)
    return out


def kernel(
    rows_ref,
    cols_ref,
    count_ref,
    tiles_ref,
    primal_ref,
    dual_ref,
    req_ref,
    ckind_ref,
    obj_ref,
    low_ref,
    up_ref,
    vkind_ref,
    pres_ref,
    dres_ref,
    met_ref,
    tiles,
    a_hi,
    a_lo,
    t_hi,
    t_lo,
    xg,
    yg,
    xo,
    yo,
    pbuf,
    part,
    tpart,
    drecv,
    precv,
    zrecv,
    zsum,
    yrecv,
    small,
    ismall,
    col_stat,
    row_stat,
    tile_sem,
    in_sem,
    gx_send,
    gx_recv,
    gy_send,
    gy_recv,
    gd_send,
    gd_recv,
    ds_send,
    ds_recv,
    ps_send,
    ps_recv,
    ts_send,
    ts_recv,
    st_send,
    st_recv,
):
    z = lax.axis_index("row_0")
    yh = lax.axis_index("row_1")
    yl = lax.axis_index("col_0")
    x = lax.axis_index("col_1")
    core = lax.axis_index("col_2")
    r_me = z * 2 + yh
    c_me = (yl * 4 + x) * 2 + core

    def up4(v, d):
        return lax.rem(v + d, 4)

    def z_dev(d):
        return (up4(z, d), yh, yl, x, core)

    def x_dev(d):
        return (z, yh, yl, up4(x, d), core)

    y_far = (z, 1 - yh, yl, x, core)
    y_near = (z, yh, 1 - yl, x, core)
    other = (z, yh, yl, x, 1 - core)

    barrier = pltpu.get_barrier_semaphore()
    near = [z_dev(d) for d in (2, 1, 3)] + [x_dev(d) for d in (2, 1, 3)] + [y_far, y_near, other]
    for dev in near:
        pl.semaphore_signal(barrier, inc=1, device_id=dev, device_id_type=MESH_ID)

    own_x = pl.ds(r_me * 8, 8)
    own_y = pl.ds(c_me * 8, 8)
    cp_x = pltpu.make_async_copy(primal_ref.reshape(8, 8, 128), xg.at[own_x], in_sem.at[0])
    cp_y = pltpu.make_async_copy(dual_ref.reshape(8, 8, 128), yg.at[own_y], in_sem.at[1])
    cp_x.start()
    cp_y.start()
    cp_x.wait()
    cp_y.wait()

    def tile_copy(t):
        return pltpu.make_async_copy(tiles_ref.at[t], tiles.at[t], tile_sem.at[t])

    for t in range(SLOTS):
        tile_copy(t).start()
    mine_r = pl.ds(pl.multiple_of(c_me * 32, 32), 32)
    mine_c = pl.ds(pl.multiple_of(r_me * 32, 32), 32)
    extra = [
        pltpu.make_async_copy(primal_ref, xo, in_sem.at[8]),
        pltpu.make_async_copy(dual_ref, yo, in_sem.at[9]),
        pltpu.make_async_copy(req_ref.at[mine_r], small.at[0], in_sem.at[2]),
        pltpu.make_async_copy(obj_ref.at[mine_c], small.at[1], in_sem.at[3]),
        pltpu.make_async_copy(low_ref.at[mine_c], small.at[2], in_sem.at[4]),
        pltpu.make_async_copy(up_ref.at[mine_c], small.at[3], in_sem.at[5]),
        pltpu.make_async_copy(ckind_ref.at[mine_r], ismall.at[0], in_sem.at[6]),
        pltpu.make_async_copy(vkind_ref.at[mine_c], ismall.at[1], in_sem.at[7]),
    ]
    for cp in extra:
        cp.start()

    lane = lax.broadcasted_iota(jnp.int32, (8, 128), 1)
    count = count_ref[0, 0]
    ridx = jnp.full((8, 128), -1, jnp.int32)
    cidx = jnp.full((8, 128), -1, jnp.int32)
    for t in range(SLOTS):
        here = (lax.rem(lane, SLOTS) == t) & (lane < 3 * SLOTS) & (jnp.full((8, 128), t, jnp.int32) < count)
        ridx = jnp.where(here, rows_ref[0, t], ridx)
        cidx = jnp.where(here, cols_ref[0, t], cidx)
    p_iota = lax.broadcasted_iota(jnp.int32, (ROW_BLOCKS, 128), 0)
    r_iota = ((p_iota // 8 % 8) * 2 + p_iota // 64) * 8 + p_iota % 8
    c_iota = lax.broadcasted_iota(jnp.int32, (COL_BLOCKS, 128), 0)
    r_hot = jnp.where(r_iota == ridx[:1], 1.0, 0.0).astype(BF16)[:, : 3 * SLOTS]
    c_hot = jnp.where(c_iota == cidx[:1], 1.0, 0.0).astype(BF16)[:, : 3 * SLOTS]

    pl.semaphore_wait(barrier, len(near))

    def send(src, dst, sems, i, dev):
        cp = pltpu.make_async_remote_copy(
            src_ref=src,
            dst_ref=dst,
            send_sem=sems[0].at[i],
            recv_sem=sems[1].at[i],
            device_id=dev,
            device_id_type=MESH_ID,
        )
        cp.start()
        return cp

    sent = []
    gx, gy, gd = (gx_send, gx_recv), (gy_send, gy_recv), (gd_send, gd_recv)

    def place(g, at, sems, i, dev):
        cp = send(g.at[pl.ds(at * 8, 8)], g.at[pl.ds(at * 8, 8)], sems, i, dev)
        sent.append(cp)
        return cp

    x_far = place(xg, r_me, gx, 0, y_far)
    x_z = [place(xg, r_me, gx, d, z_dev(d)) for d in (2, 1, 3)]
    y_n = place(yg, c_me, gy, 0, y_near)
    y_x = {d: place(yg, c_me, gy, d, x_dev(d)) for d in (2, 1, 3)}
    y_d = [place(yg, c_me, gd, 0, other)]

    def convert(t, carry):
        tile_copy(t).wait()

        def piece(i, c):
            sl = pl.ds(pl.multiple_of(i * 128, 128), 128)
            v = tiles[t, sl, :]
            hi, lo = split2(v)
            a_hi[t, sl, :] = hi
            a_lo[t, sl, :] = lo
            hi, lo = split2(v.T)
            t_hi[t, :, sl] = hi
            t_lo[t, :, sl] = lo
            return c

        return lax.fori_loop(0, BLK // 128, piece, carry, unroll=True)

    lax.fori_loop(0, 7, convert, 0)
    y_n.wait_recv()
    at = ((1 - yl) * 4 + x) * 2 + core
    y_x2 = {d: place(yg, at, gy, 3 + d, x_dev(d)) for d in (2, 1, 3)}
    y_d.append(place(yg, at, gd, 1, other))
    lax.fori_loop(7, 11, convert, 0)
    x_far.wait_recv()
    at = z * 2 + 1 - yh
    x_z2 = [place(xg, at, gx, 3 + d, z_dev(d)) for d in (2, 1, 3)]
    for d in (1, 3, 2):
        y_x[d].wait_recv()
        at = (yl * 4 + up4(x, 4 - d)) * 2 + core
        y_d.append(place(yg, at, gd, 1 + d, other))
    lax.fori_loop(11, 16, convert, 0)
    for d in (1, 3, 2):
        y_x2[d].wait_recv()
        at = ((1 - yl) * 4 + up4(x, 4 - d)) * 2 + core
        y_d.append(place(yg, at, gd, 4 + d, other))

    def scatter(hot, dest, blocks):
        cols = []
        for e in range(8):
            v = pbuf[pl.ds(e, SLOTS, stride=8), :]
            hi = v.astype(BF16)
            rest = v - hi.astype(F32)
            mid = rest.astype(BF16)
            lo = (rest - mid.astype(F32)).astype(BF16)
            cols.append(jnp.concatenate([hi, mid, lo], axis=0))
        rhs = jnp.concatenate(cols, axis=1)
        out = jnp.dot(hot, rhs, preferred_element_type=F32)
        for e in range(8):
            dest[pl.ds(e, blocks, stride=8), :] = out[:, e * 128 : (e + 1) * 128]

    def products(first, count, grouped, vec, index, hi_ref, lo_ref):
        def body(i, carry):
            for j in range(grouped):
                t = first + i * grouped + j
                lhs = spread(vec[index[0, t]])
                res = jnp.dot(lhs, hi_ref[t], preferred_element_type=F32)
                res = res + jnp.dot(lhs, lo_ref[t], preferred_element_type=F32)
                pbuf[pl.ds(pl.multiple_of(t * 8, 8), 8), :] = gathered(res)
            return carry

        lax.fori_loop(0, count // grouped, body, 0)

    dsem, psem, tsem, ssem = (ds_send, ds_recv), (ps_send, ps_recv), (ts_send, ts_recv), (st_send, st_recv)

    def z_rows(v):
        return pl.ds(pl.multiple_of(v * 2 * OWN, 2 * OWN), 2 * OWN)

    def share(c, off):
        chip = lax.rem(yl + off[0], 2) * 4 + up4(x, off[1])
        return pl.ds(pl.multiple_of((c * 8 + chip) * OWN, OWN), OWN)

    for cp in y_d:
        cp.wait_recv()
    products(0, SLOTS, 4, yg, rows_ref, a_hi, a_lo)
    scatter(c_hot, tpart, COL_BLOCKS)
    z_rs = []
    for i, d in enumerate((2, 1, 3)):
        z_rs.append(send(tpart.at[z_rows(up4(z, d))], zrecv.at[i], tsem, i, z_dev(d)))
    for cp in x_z + x_z2:
        cp.wait_recv()
    products(0, SLOTS, 4, xg, cols_ref, t_hi, t_lo)
    scatter(r_hot, part, ROW_BLOCKS)
    d_rs = []
    for i, off in enumerate(CHIP_OFFS):
        d_rs.append(send(part.at[share(1 - core, off)], drecv.at[i], dsem, i, other))
    p_rs = []
    for i, off in enumerate(CHIP_OFFS):
        d_rs[i].wait_recv()
        mine = share(core, off)
        part[mine, :] = part[mine, :] + drecv[i]
        if i < 7:
            dev = (z, yh, lax.rem(yl + off[0], 2), up4(x, off[1]), core)
            p_rs.append(send(part.at[mine], precv.at[i], psem, i, dev))
    for cp in extra:
        cp.wait()
    for cp in z_rs:
        cp.wait_recv()
    zsum[...] = tpart[z_rows(z), :] + zrecv[0] + zrecv[1] + zrecv[2]
    half = pl.ds(pl.multiple_of((1 - yh) * OWN, OWN), OWN)
    y_rs = send(zsum.at[half], yrecv, tsem, 3, y_far)
    dual_own = [yo[pl.ds(s, 32, stride=2), :] for s in range(2)]
    primal_own = [xo[pl.ds(s, 32, stride=2), :] for s in range(2)]
    stat_rows = [[], []]

    def total(v):
        return jnp.sum(v.reshape(4, 8, 128), axis=0)

    y_rs.wait_recv()
    dres_ref[...] = zsum[pl.ds(pl.multiple_of(yh * OWN, OWN), OWN), :] + yrecv[...]
    obj, low, up, vk = small[1], small[2], small[3], ismall[1]
    low_on = (vk == 1) | (vk == 3)
    up_on = (vk == 2) | (vk == 3)
    for s in range(2):
        reduced = obj - dres_ref[pl.ds(s, 32, stride=2), :]
        mult = jnp.where(low_on, jnp.maximum(reduced, 0.0), 0.0) + jnp.where(
            up_on, jnp.minimum(reduced, 0.0), 0.0
        )
        res = reduced - mult
        dres_ref[pl.ds(s, 32, stride=2), :] = res
        bound = low * jnp.maximum(mult, 0.0) + up * jnp.minimum(mult, 0.0)
        stat_rows[s] += [
            total(res * res),
            total(obj * obj),
            total(obj * primal_own[s]),
            total(bound),
        ]
    for cp in p_rs:
        cp.wait_recv()
    product = part[share(core, (0, 0)), :]
    for i in range(7):
        product = product + precv[i]
    pres_ref[...] = product
    req = small[0]
    is_ge = ismall[0] == 1
    for s in range(2):
        diff = req - pres_ref[pl.ds(s, 32, stride=2), :]
        res = jnp.where(is_ge, jnp.maximum(diff, 0.0), diff)
        pres_ref[pl.ds(s, 32, stride=2), :] = res
        stat_rows[s] += [total(res * res), total(req * req), total(req * dual_own[s])]

    lane1 = lax.broadcasted_iota(jnp.int32, (1, 128), 1)
    for s in range(2):
        acc = jnp.zeros((1, 128), F32)
        for q in range(7):
            v = jnp.sum(stat_rows[s][q], axis=0, keepdims=True)
            v = jnp.sum(v, axis=1, keepdims=True)
            acc = jnp.where(lane1 == q, v, acc)
        col_stat[c_me, pl.ds(s, 1), :] = acc

    stat = []
    for dy, dx in CHIP_OFFS:
        for dc in range(2):
            if (dy, dx, dc) != (0, 0, 0):
                dev = (z, yh, lax.rem(yl + dy, 2), up4(x, dx), lax.rem(core + dc, 2))
                stat.append(send(col_stat.at[c_me], col_stat.at[c_me], ssem, len(stat), dev))
    for cp in stat:
        cp.wait_recv()
    row_stat[r_me] = jnp.sum(col_stat[...], axis=0)
    rstat = []
    for d in (2, 1, 3, 0):
        for dy in (1, 0):
            if (d, dy) != (0, 0):
                dev = (up4(z, d), lax.rem(yh + dy, 2), yl, x, core)
                rstat.append(send(row_stat.at[r_me], row_stat.at[r_me], ssem, 15 + len(rstat), dev))
    for cp in rstat:
        cp.wait_recv()
    acc = jnp.sum(row_stat[...], axis=0)

    pick = [acc[:, q : q + 1] for q in range(7)]
    primal_square, require_square, require_dot = pick[4], pick[5], pick[6]
    dual_square, objective_square, objective_dot, bound_sum = pick[0], pick[1], pick[2], pick[3]
    primal_ratio = jnp.sqrt(primal_square) / (1.0 + jnp.sqrt(require_square))
    dual_ratio = jnp.sqrt(dual_square) / (1.0 + jnp.sqrt(objective_square))
    dual_value = require_dot + bound_sum
    gap = jnp.abs(objective_dot - dual_value) / (1.0 + jnp.abs(objective_dot) + jnp.abs(dual_value))
    lane2 = lax.broadcasted_iota(jnp.int32, (2, 128), 1)
    met = jnp.where(lane2 == 0, primal_ratio, jnp.where(lane2 == 1, dual_ratio, gap))
    met_ref[...] = met[:, :3]

    for cp in sent + d_rs + p_rs + z_rs + [y_rs] + stat + rstat:
        cp.wait_send()


def flush(a, b, c, a_out, b_out, c_out, sem):
    copies = [
        pltpu.make_async_copy(src, dst, sem.at[i])
        for i, (src, dst) in enumerate(((a, a_out), (b, b_out), (c, c_out)))
    ]
    for cp in copies:
        cp.start()
    for cp in copies:
        cp.wait()


def interleave(a):
    return a.reshape(2, 32, 128).transpose(1, 0, 2).reshape(OWN, 128)


def deinterleave(a):
    return a.reshape(32, 2, 128).transpose(1, 0, 2).reshape(2, 4096)


def on_device(
    matrix_tiles,
    tile_rows,
    tile_columns,
    tile_counts,
    primal_iter,
    dual_iter,
    requirement,
    constraint_kind,
    objective,
    lower_bound,
    upper_bound,
    variable_kind,
):
    hbm = pl.BlockSpec(memory_space=pl.ANY)
    smem = pl.BlockSpec(memory_space=pltpu.SMEM)
    vmem = pl.BlockSpec(memory_space=pltpu.VMEM)
    dma = pltpu.SemaphoreType.DMA
    pres, dres, metrics = pl.pallas_call(
        kernel,
        name="restart_check",
        out_shape=(
            pltpu.VMEM((OWN, 128), F32),
            pltpu.VMEM((OWN, 128), F32),
            pltpu.VMEM((2, 3), F32),
        ),
        in_specs=[smem] * 3 + [hbm] * 9,
        out_specs=(vmem, vmem, vmem),
        scratch_shapes=[
            pltpu.VMEM((SLOTS, BLK, BLK), F32),
            pltpu.VMEM((SLOTS, BLK, BLK), BF16),
            pltpu.VMEM((SLOTS, BLK, BLK), BF16),
            pltpu.VMEM((SLOTS, BLK, BLK), BF16),
            pltpu.VMEM((SLOTS, BLK, BLK), BF16),
            pltpu.VMEM((COL_BLOCKS, 8, 128), F32),
            pltpu.VMEM((ROW_BLOCKS, 8, 128), F32),
            pltpu.VMEM((OWN, 128), F32),
            pltpu.VMEM((OWN, 128), F32),
            pltpu.VMEM((SLOTS * 8, 128), F32),
            pltpu.VMEM((16 * OWN, 128), F32),
            pltpu.VMEM((8 * OWN, 128), F32),
            pltpu.VMEM((8, OWN, 128), F32),
            pltpu.VMEM((7, OWN, 128), F32),
            pltpu.VMEM((3, 2 * OWN, 128), F32),
            pltpu.VMEM((2 * OWN, 128), F32),
            pltpu.VMEM((OWN, 128), F32),
            pltpu.VMEM((4, 32, 128), F32),
            pltpu.VMEM((2, 32, 128), jnp.int32),
            pltpu.VMEM((16, 2, 128), F32),
            pltpu.VMEM((8, 2, 128), F32),
            dma((SLOTS,)),
            dma((10,)),
            dma((7,)),
            dma((7,)),
            dma((7,)),
            dma((7,)),
            dma((8,)),
            dma((8,)),
            dma((8,)),
            dma((8,)),
            dma((7,)),
            dma((7,)),
            dma((4,)),
            dma((4,)),
            dma((22,)),
            dma((22,)),
        ],
        compiler_params=pltpu.CompilerParams(
            collective_id=0, has_side_effects=True, vmem_limit_bytes=60 * 1024 * 1024
        ),
    )(
        tile_rows.reshape(1, SLOTS),
        tile_columns.reshape(1, SLOTS),
        tile_counts,
        matrix_tiles.reshape(SLOTS, BLK, BLK),
        interleave(primal_iter),
        interleave(dual_iter),
        requirement.reshape(512, 128),
        constraint_kind.reshape(512, 128),
        objective.reshape(256, 128),
        lower_bound.reshape(256, 128),
        upper_bound.reshape(256, 128),
        variable_kind.reshape(256, 128),
    )
    pres, dres, metrics = pl.pallas_call(
        flush,
        name="flush",
        out_shape=(
            pltpu.HBM((OWN, 128), F32),
            pltpu.HBM((OWN, 128), F32),
            pltpu.HBM((2, 3), F32),
        ),
        in_specs=[vmem] * 3,
        out_specs=(hbm,) * 3,
        scratch_shapes=[dma((3,))],
        compiler_params=pltpu.CompilerParams(vmem_limit_bytes=1024 * 1024),
    )(pres, dres, metrics)
    return deinterleave(pres), deinterleave(dres), metrics


def solution(mesh):
    torus = Mesh(mesh.devices.reshape(4, 2, 2, 4, 2), ROW_COL)
    return jax.shard_map(
        on_device,
        mesh=torus,
        in_specs=(
            P(ROW, COL, None, None, None),
            P(ROW, COL, None),
            P(ROW, COL, None),
            P(ROW, COL),
            P(None, COL_ROW),
            P(None, ROW_COL),
            P(ROW),
            P(ROW),
            P(COL),
            P(COL),
            P(COL),
            P(COL),
        ),
        out_specs=(P(None, ROW_COL), P(None, COL_ROW), P()),
        check_vma=False,
    )
```

```python
import jax
import jax.numpy as jnp
from jax import lax
from jax.experimental import pallas as pl
from jax.experimental.pallas import tpu as pltpu
from jax.sharding import Mesh
from jax.sharding import PartitionSpec as P

ROW = ("row_0", "row_1")
COL = ("col_0", "col_1", "col_2")
ROW_COL = ROW + COL
COL_ROW = COL + ROW
MESH_ID = pl.DeviceIdType.MESH

BLK = 512
SLOTS = 16
ROW_BLOCKS = 128
COL_BLOCKS = 64
UNROLL = 16
OWN = 64

CHIP_OFFS = [(1, 2), (1, 1), (1, 3), (0, 2), (1, 0), (0, 1), (0, 3), (0, 0)]
GROUPS = 4
RECV = ["x_far", "x_z", "y_n", "y_x", "y_x2", "y_d", "z_rs", "y_rs", "p_rs", "stat"]


def hops(off):
    dz, dh, dl, dx, dc = off
    return min(dz, 4 - dz) + min(dx, 4 - dx) + (2 * dh if not dl else 1) + 0.2 * dc


PEERS = [
    (dz, dh, dl, dx, dc)
    for dz in range(4)
    for dh in range(2)
    for dl in range(2)
    for dx in range(4)
    for dc in range(2)
]
PEERS = sorted(PEERS[1:], key=hops, reverse=True)
F32 = jnp.float32
BF16 = jnp.bfloat16


def split2(v):
    hi = v.astype(BF16)
    lo = (v - hi.astype(F32)).astype(BF16)
    return hi, lo


def spread(v):
    sub = lax.broadcasted_iota(jnp.int32, (8, 128), 0)
    hi = v.astype(BF16).astype(F32)
    lo = v - hi
    parts = []
    for k in range(4):
        keep = (sub // 2) == k
        parts.append(jnp.concatenate([jnp.where(keep, hi, 0.0), jnp.where(keep, lo, 0.0)], axis=0))
    return jnp.concatenate(parts, axis=1).astype(BF16)


def gathered(r):
    sub = lax.broadcasted_iota(jnp.int32, (8, 128), 0)
    out = jnp.zeros((8, 128), F32)
    for g in range(4):
        c = r[:8, 128 * g : 128 * g + 128] + r[8:, 128 * g : 128 * g + 128]
        c = c + pltpu.roll(c, 2, 0)
        c = c + pltpu.roll(c, 4, 0)
        out = jnp.where((sub // 2) == g, c, out)
    return out


def kernel(
    rows_hbm,
    cols_hbm,
    count_hbm,
    tiles_ref,
    primal_ref,
    dual_ref,
    req_ref,
    ckind_ref,
    obj_ref,
    low_ref,
    up_ref,
    vkind_ref,
    pres_ref,
    dres_ref,
    met_ref,
    tab,
    count_ref,
    tiles,
    a_hi,
    a_lo,
    t_hi,
    t_lo,
    xg,
    yg,
    pbuf,
    part,
    tpart,
    drecv,
    precv,
    zrecv,
    zsum,
    yrecv,
    small,
    ismall,
    stats,
    tile_sem,
    in_sem,
    sent_sem,
    recv_sem,
    d_recv,
):
    z = lax.axis_index("row_0")
    yh = lax.axis_index("row_1")
    yl = lax.axis_index("col_0")
    x = lax.axis_index("col_1")
    core = lax.axis_index("col_2")
    r_me = z * 2 + yh
    c_me = (yl * 4 + x) * 2 + core

    def up4(v, d):
        return lax.rem(v + d, 4)

    def z_dev(d):
        return (up4(z, d), yh, yl, x, core)

    def x_dev(d):
        return (z, yh, yl, up4(x, d), core)

    y_far = (z, 1 - yh, yl, x, core)
    y_near = (z, yh, 1 - yl, x, core)
    other = (z, yh, yl, x, 1 - core)

    def whole(ref, sem):
        pltpu.make_async_copy(ref, ref, sem).wait()

    barrier = pltpu.get_barrier_semaphore()
    near = [z_dev(d) for d in (2, 1, 3)] + [x_dev(d) for d in (2, 1, 3)] + [y_far, y_near, other]
    for dev in near:
        pl.semaphore_signal(barrier, inc=1, device_id=dev, device_id_type=MESH_ID)

    own_x = pl.ds(r_me * 8, 8)
    own_y = pl.ds(c_me * 8, 8)
    cp_x = pltpu.make_async_copy(primal_ref.reshape(8, 8, 128), xg.at[own_x], in_sem.at[0])
    cp_y = pltpu.make_async_copy(dual_ref.reshape(8, 8, 128), yg.at[own_y], in_sem.at[1])
    cp_x.start()
    cp_y.start()
    tables = [
        pltpu.make_async_copy(rows_hbm, tab.at[0], in_sem.at[4]),
        pltpu.make_async_copy(cols_hbm, tab.at[1], in_sem.at[4]),
        pltpu.make_async_copy(count_hbm, count_ref, in_sem.at[5]),
    ]
    for cp in tables:
        cp.start()
    cp_x.wait()
    cp_y.wait()

    def tile_copy(g):
        four = pl.ds(g * (SLOTS // GROUPS), SLOTS // GROUPS)
        return pltpu.make_async_copy(tiles_ref.at[four], tiles.at[four], tile_sem.at[g])

    for g in range(GROUPS):
        tile_copy(g).start()
    mine_r = pl.ds(pl.multiple_of(c_me * 32, 32), 32)
    mine_c = pl.ds(pl.multiple_of(r_me * 32, 32), 32)
    extra = [
        pltpu.make_async_copy(req_ref.at[mine_r], small.at[0], in_sem.at[2]),
        pltpu.make_async_copy(obj_ref.at[mine_c], small.at[1], in_sem.at[2]),
        pltpu.make_async_copy(low_ref.at[mine_c], small.at[2], in_sem.at[2]),
        pltpu.make_async_copy(up_ref.at[mine_c], small.at[3], in_sem.at[2]),
        pltpu.make_async_copy(ckind_ref.at[mine_r], ismall.at[0], in_sem.at[3]),
        pltpu.make_async_copy(vkind_ref.at[mine_c], ismall.at[1], in_sem.at[3]),
    ]
    for cp in extra:
        cp.start()

    whole(tab, in_sem.at[4])
    tables[2].wait()
    lane = lax.broadcasted_iota(jnp.int32, (8, 128), 1)
    count = count_ref[0, 0]
    ridx = jnp.full((8, 128), -1, jnp.int32)
    cidx = jnp.full((8, 128), -1, jnp.int32)
    for t in range(SLOTS):
        here = (lax.rem(lane, SLOTS) == t) & (lane < 3 * SLOTS) & (jnp.full((8, 128), t, jnp.int32) < count)
        ridx = jnp.where(here, tab[0, 0, t], ridx)
        cidx = jnp.where(here, tab[1, 0, t], cidx)
    p_iota = lax.broadcasted_iota(jnp.int32, (ROW_BLOCKS, 128), 0)
    r_iota = ((p_iota // 8 % 8) * 2 + p_iota // 64) * 8 + p_iota % 8
    c_iota = lax.broadcasted_iota(jnp.int32, (COL_BLOCKS, 128), 0)
    r_hot = jnp.where(r_iota == ridx[:1], 1.0, 0.0).astype(BF16)[:, : 3 * SLOTS]
    c_hot = jnp.where(c_iota == cidx[:1], 1.0, 0.0).astype(BF16)[:, : 3 * SLOTS]

    pl.semaphore_wait(barrier, len(near))

    def send(src, dst, phase, recv, dev):
        cp = pltpu.make_async_remote_copy(
            src_ref=src,
            dst_ref=dst,
            send_sem=sent_sem.at[phase],
            recv_sem=recv if not isinstance(recv, str) else recv_sem.at[RECV.index(recv)],
            device_id=dev,
            device_id_type=MESH_ID,
        )
        cp.start()
        return cp

    def arrived(ref, name):
        whole(ref, recv_sem.at[RECV.index(name)])

    def place(g, at, recv, dev):
        send(g.at[pl.ds(at * 8, 8)], g.at[pl.ds(at * 8, 8)], 0, recv, dev)

    place(xg, r_me, "x_far", y_far)
    for d in (2, 1, 3):
        place(xg, r_me, "x_z", z_dev(d))
    place(yg, c_me, "y_n", y_near)
    for d in (2, 1, 3):
        place(yg, c_me, "y_x", x_dev(d))
    place(yg, c_me, "y_d", other)

    def convert(t, carry):
        def piece(i, c):
            sl = pl.ds(pl.multiple_of(i * 128, 128), 128)
            v = tiles[t, sl, :]
            hi, lo = split2(v)
            a_hi[t, sl, :] = hi
            a_lo[t, sl, :] = lo
            hi, lo = split2(v.T)
            t_hi[t, :, sl] = hi
            t_lo[t, :, sl] = lo
            return c

        return lax.fori_loop(0, BLK // 128, piece, carry, unroll=True)

    tile_copy(0).wait()
    lax.fori_loop(0, 4, convert, 0)
    tile_copy(1).wait()
    lax.fori_loop(4, 7, convert, 0)
    arrived(yg.at[pl.ds(0, 8)], "y_n")
    at = ((1 - yl) * 4 + x) * 2 + core
    for d in (2, 1, 3):
        place(yg, at, "y_x2", x_dev(d))
    place(yg, at, "y_d", other)
    tile_copy(2).wait()
    lax.fori_loop(7, 11, convert, 0)
    arrived(xg.at[pl.ds(0, 8)], "x_far")
    for d in (2, 1, 3):
        place(xg, z * 2 + 1 - yh, "x_z", z_dev(d))
    arrived(yg.at[pl.ds(0, 24)], "y_x")
    for d in (1, 3, 2):
        place(yg, (yl * 4 + up4(x, d)) * 2 + core, "y_d", other)
    tile_copy(3).wait()
    lax.fori_loop(11, 16, convert, 0)
    arrived(yg.at[pl.ds(0, 24)], "y_x2")
    for d in (1, 3, 2):
        place(yg, ((1 - yl) * 4 + up4(x, d)) * 2 + core, "y_d", other)

    def scatter(hot, dest, blocks):
        cols = []
        for e in range(8):
            v = pbuf[pl.ds(e, SLOTS, stride=8), :]
            hi = v.astype(BF16)
            rest = v - hi.astype(F32)
            mid = rest.astype(BF16)
            lo = (rest - mid.astype(F32)).astype(BF16)
            cols.append(jnp.concatenate([hi, mid, lo], axis=0))
        rhs = jnp.concatenate(cols, axis=1)
        out = jnp.dot(hot, rhs, preferred_element_type=F32)
        for e in range(8):
            dest[pl.ds(e, blocks, stride=8), :] = out[:, e * 128 : (e + 1) * 128]

    def products(first, count, grouped, vec, index, hi_ref, lo_ref):
        def body(i, carry):
            for j in range(grouped):
                t = first + i * grouped + j
                lhs = spread(vec[tab[index, 0, t]])
                res = jnp.dot(lhs, hi_ref[t], preferred_element_type=F32)
                res = res + jnp.dot(lhs, lo_ref[t], preferred_element_type=F32)
                pbuf[pl.ds(pl.multiple_of(t * 8, 8), 8), :] = gathered(res)
            return carry

        lax.fori_loop(0, count // grouped, body, 0)


    def z_rows(v):
        return pl.ds(pl.multiple_of(v * 2 * OWN, 2 * OWN), 2 * OWN)

    def share(c, off):
        chip = lax.rem(yl + off[0], 2) * 4 + up4(x, off[1])
        return pl.ds(pl.multiple_of((c * 8 + chip) * OWN, OWN), OWN)

    arrived(yg.at[pl.ds(0, 64)], "y_d")
    products(0, SLOTS, UNROLL, yg, 0, a_hi, a_lo)
    scatter(c_hot, tpart, COL_BLOCKS)
    for i, d in enumerate((2, 1, 3)):
        send(tpart.at[z_rows(up4(z, d))], zrecv.at[i], 1, "z_rs", z_dev(d))
    arrived(xg.at[pl.ds(0, 48)], "x_z")
    products(0, SLOTS, UNROLL, xg, 1, t_hi, t_lo)
    scatter(r_hot, part, ROW_BLOCKS)
    d_rs = []
    for i, off in enumerate(CHIP_OFFS):
        d_rs.append(send(part.at[share(1 - core, off)], drecv.at[i], 1, d_recv.at[i], other))
    for i, off in enumerate(CHIP_OFFS):
        d_rs[i].wait_recv()
        mine = share(core, off)
        part[mine, :] = part[mine, :] + drecv[i]
        if i < 7:
            dev = (z, yh, lax.rem(yl + off[0], 2), up4(x, off[1]), core)
            send(part.at[mine], precv.at[i], 1, "p_rs", dev)
    whole(small, in_sem.at[2])
    whole(ismall, in_sem.at[3])
    arrived(zrecv, "z_rs")
    zsum[...] = tpart[z_rows(z), :] + zrecv[0] + zrecv[1] + zrecv[2]
    half = pl.ds(pl.multiple_of((1 - yh) * OWN, OWN), OWN)
    send(zsum.at[half], yrecv, 1, "y_rs", y_far)
    dual_own = [yg.reshape(ROW_BLOCKS * 8, 128)[pl.ds(c_me * OWN + s, 32, stride=2), :] for s in range(2)]
    primal_own = [xg.reshape(COL_BLOCKS * 8, 128)[pl.ds(r_me * OWN + s, 32, stride=2), :] for s in range(2)]
    stat_rows = [[], []]

    def total(v):
        return jnp.sum(v.reshape(4, 8, 128), axis=0)

    arrived(yrecv, "y_rs")
    dres_ref[...] = zsum[pl.ds(pl.multiple_of(yh * OWN, OWN), OWN), :] + yrecv[...]
    obj, low, up, vk = small[1], small[2], small[3], ismall[1]
    low_on = (vk == 1) | (vk == 3)
    up_on = (vk == 2) | (vk == 3)
    for s in range(2):
        reduced = obj - dres_ref[pl.ds(s, 32, stride=2), :]
        mult = jnp.where(low_on, jnp.maximum(reduced, 0.0), 0.0) + jnp.where(
            up_on, jnp.minimum(reduced, 0.0), 0.0
        )
        res = reduced - mult
        dres_ref[pl.ds(s, 32, stride=2), :] = res
        bound = low * jnp.maximum(mult, 0.0) + up * jnp.minimum(mult, 0.0)
        stat_rows[s] += [
            total(res * res),
            total(obj * obj),
            total(obj * primal_own[s]),
            total(bound),
        ]
    arrived(precv, "p_rs")
    product = part[share(core, (0, 0)), :]
    for i in range(7):
        product = product + precv[i]
    pres_ref[...] = product
    req = small[0]
    is_ge = ismall[0] == 1
    for s in range(2):
        diff = req - pres_ref[pl.ds(s, 32, stride=2), :]
        res = jnp.where(is_ge, jnp.maximum(diff, 0.0), diff)
        pres_ref[pl.ds(s, 32, stride=2), :] = res
        stat_rows[s] += [total(res * res), total(req * req), total(req * dual_own[s])]

    lane1 = lax.broadcasted_iota(jnp.int32, (1, 128), 1)
    acc = jnp.zeros((1, 128), F32)
    for s in range(2):
        for q in range(7):
            v = jnp.sum(stat_rows[s][q], axis=0, keepdims=True)
            v = jnp.sum(v, axis=1, keepdims=True)
            acc = jnp.where(lane1 == 7 * s + q, v, acc)
    me = r_me * 16 + c_me
    stats[me] = acc
    for dz, dh, dl, dx, dc in PEERS:
        dev = (up4(z, dz), lax.rem(yh + dh, 2), lax.rem(yl + dl, 2), up4(x, dx), lax.rem(core + dc, 2))
        send(stats.at[me], stats.at[me], 2, "stat", dev)
    arrived(stats.at[pl.ds(0, 127)], "stat")
    acc = jnp.sum(stats[...], axis=0)

    pick = [jnp.concatenate([acc[:, q : q + 1], acc[:, 7 + q : 8 + q]], axis=0) for q in range(7)]
    primal_square, require_square, require_dot = pick[4], pick[5], pick[6]
    dual_square, objective_square, objective_dot, bound_sum = pick[0], pick[1], pick[2], pick[3]
    primal_ratio = jnp.sqrt(primal_square) / (1.0 + jnp.sqrt(require_square))
    dual_ratio = jnp.sqrt(dual_square) / (1.0 + jnp.sqrt(objective_square))
    dual_value = require_dot + bound_sum
    gap = jnp.abs(objective_dot - dual_value) / (1.0 + jnp.abs(objective_dot) + jnp.abs(dual_value))
    lane2 = lax.broadcasted_iota(jnp.int32, (2, 128), 1)
    met = jnp.where(lane2 == 0, primal_ratio, jnp.where(lane2 == 1, dual_ratio, gap))
    met_ref[...] = met[:, :3]

    whole(tiles.at[0, pl.ds(0, 352)], sent_sem.at[0])
    whole(tiles.at[0, pl.ds(0, 352)], sent_sem.at[1])
    whole(stats.at[pl.ds(0, 127)], sent_sem.at[2])


def flush(a, b, c, a_out, b_out, c_out, sem):
    copies = [
        pltpu.make_async_copy(src, dst, sem.at[i])
        for i, (src, dst) in enumerate(((a, a_out), (b, b_out), (c, c_out)))
    ]
    for cp in copies:
        cp.start()
    for cp in copies:
        cp.wait()


def interleave(a):
    return a.reshape(2, 32, 128).transpose(1, 0, 2).reshape(OWN, 128)


def deinterleave(a):
    return a.reshape(32, 2, 128).transpose(1, 0, 2).reshape(2, 4096)


def on_device(
    matrix_tiles,
    tile_rows,
    tile_columns,
    tile_counts,
    primal_iter,
    dual_iter,
    requirement,
    constraint_kind,
    objective,
    lower_bound,
    upper_bound,
    variable_kind,
):
    hbm = pl.BlockSpec(memory_space=pl.ANY)
    vmem = pl.BlockSpec(memory_space=pltpu.VMEM)
    dma = pltpu.SemaphoreType.DMA
    pres, dres, metrics = pl.pallas_call(
        kernel,
        name="restart_check",
        out_shape=(
            pltpu.VMEM((OWN, 128), F32),
            pltpu.VMEM((OWN, 128), F32),
            pltpu.VMEM((2, 3), F32),
        ),
        in_specs=[hbm] * 12,
        out_specs=(vmem, vmem, vmem),
        scratch_shapes=[
            pltpu.SMEM((2, 1, SLOTS), jnp.int32),
            pltpu.SMEM((1, 1), jnp.int32),
            pltpu.VMEM((SLOTS, BLK, BLK), F32),
            pltpu.VMEM((SLOTS, BLK, BLK), BF16),
            pltpu.VMEM((SLOTS, BLK, BLK), BF16),
            pltpu.VMEM((SLOTS, BLK, BLK), BF16),
            pltpu.VMEM((SLOTS, BLK, BLK), BF16),
            pltpu.VMEM((COL_BLOCKS, 8, 128), F32),
            pltpu.VMEM((ROW_BLOCKS, 8, 128), F32),
            pltpu.VMEM((SLOTS * 8, 128), F32),
            pltpu.VMEM((16 * OWN, 128), F32),
            pltpu.VMEM((8 * OWN, 128), F32),
            pltpu.VMEM((8, OWN, 128), F32),
            pltpu.VMEM((7, OWN, 128), F32),
            pltpu.VMEM((3, 2 * OWN, 128), F32),
            pltpu.VMEM((2 * OWN, 128), F32),
            pltpu.VMEM((OWN, 128), F32),
            pltpu.VMEM((4, 32, 128), F32),
            pltpu.VMEM((2, 32, 128), jnp.int32),
            pltpu.VMEM((128, 1, 128), F32),
            dma((GROUPS,)),
            dma((6,)),
            dma((3,)),
            dma((len(RECV),)),
            dma((8,)),
        ],
        compiler_params=pltpu.CompilerParams(
            collective_id=0, has_side_effects=True, vmem_limit_bytes=60 * 1024 * 1024
        ),
    )(
        tile_rows.reshape(1, SLOTS),
        tile_columns.reshape(1, SLOTS),
        tile_counts,
        matrix_tiles.reshape(SLOTS, BLK, BLK),
        interleave(primal_iter),
        interleave(dual_iter),
        requirement.reshape(512, 128),
        constraint_kind.reshape(512, 128),
        objective.reshape(256, 128),
        lower_bound.reshape(256, 128),
        upper_bound.reshape(256, 128),
        variable_kind.reshape(256, 128),
    )
    pres, dres, metrics = pl.pallas_call(
        flush,
        name="flush",
        out_shape=(
            pltpu.HBM((OWN, 128), F32),
            pltpu.HBM((OWN, 128), F32),
            pltpu.HBM((2, 3), F32),
        ),
        in_specs=[vmem] * 3,
        out_specs=(hbm,) * 3,
        scratch_shapes=[dma((3,))],
        compiler_params=pltpu.CompilerParams(vmem_limit_bytes=1024 * 1024),
    )(pres, dres, metrics)
    return deinterleave(pres), deinterleave(dres), metrics


def solution(mesh):
    torus = Mesh(mesh.devices.reshape(4, 2, 2, 4, 2), ROW_COL)
    return jax.shard_map(
        on_device,
        mesh=torus,
        in_specs=(
            P(ROW, COL, None, None, None),
            P(ROW, COL, None),
            P(ROW, COL, None),
            P(ROW, COL),
            P(None, COL_ROW),
            P(None, ROW_COL),
            P(ROW),
            P(ROW),
            P(COL),
            P(COL),
            P(COL),
            P(COL),
        ),
        out_specs=(P(None, ROW_COL), P(None, COL_ROW), P()),
        check_vma=False,
    )
```

```python
import jax
import jax.numpy as jnp
from jax import lax
from jax.experimental import pallas as pl
from jax.experimental.pallas import tpu as pltpu
from jax.sharding import Mesh
from jax.sharding import PartitionSpec as P

ROW = ("row_0", "row_1")
COL = ("col_0", "col_1", "col_2")
ROW_COL = ROW + COL
COL_ROW = COL + ROW
MESH_ID = pl.DeviceIdType.MESH

BLK = 512
SLOTS = 16
ROW_BLOCKS = 128
COL_BLOCKS = 64
HALF = 512
OWN = 64

CHIP_OFFS = [(1, 2), (1, 1), (1, 3), (0, 2), (1, 0), (0, 1), (0, 3), (0, 0)]
VECTOR = [1, 3, 5, 7, 9, 11, 13]
MATRIX = [t for t in range(SLOTS) if t not in VECTOR]
BATCHES = [(0, 3), (3, 6), (6, 9), (9, 12), (12, 16)]
RECV = ["x_far", "x_z", "y_n", "y_x", "y_x2", "y_d", "d_0", "d_1", "z_far", "z_near", "y_rs", "p_rs", "stat"]


def hops(off):
    dz, dh, dl, dx, dc = off
    return min(dz, 4 - dz) + min(dx, 4 - dx) + (2 * dh if not dl else 1) + 0.2 * dc


PEERS = [
    (dz, dh, dl, dx, dc)
    for dz in range(4)
    for dh in range(2)
    for dl in range(2)
    for dx in range(4)
    for dc in range(2)
]
PEERS = sorted(PEERS[1:], key=hops, reverse=True)
F32 = jnp.float32
BF16 = jnp.bfloat16


def split2(v):
    hi = v.astype(BF16)
    lo = (v - hi.astype(F32)).astype(BF16)
    return hi, lo


def spread(v):
    sub = lax.broadcasted_iota(jnp.int32, (8, 128), 0)
    hi = v.astype(BF16).astype(F32)
    lo = v - hi
    parts = []
    for k in range(4):
        keep = (sub // 2) == k
        parts.append(jnp.concatenate([jnp.where(keep, hi, 0.0), jnp.where(keep, lo, 0.0)], axis=0))
    return jnp.concatenate(parts, axis=1).astype(BF16)


def gathered(r, groups):
    sub = lax.broadcasted_iota(jnp.int32, (8, 128), 0)
    out = jnp.zeros((8, 128), F32)
    for i, g in enumerate(groups):
        c = r[:8, 128 * i : 128 * i + 128] + r[8:, 128 * i : 128 * i + 128]
        c = c + pltpu.roll(c, 2, 0)
        c = c + pltpu.roll(c, 4, 0)
        out = jnp.where((sub // 2) == g, c, out)
    return out


def kernel(
    rows_hbm,
    cols_hbm,
    count_hbm,
    tiles_ref,
    primal_ref,
    dual_ref,
    req_ref,
    ckind_ref,
    obj_ref,
    low_ref,
    up_ref,
    vkind_ref,
    pres_ref,
    dres_ref,
    met_ref,
    tab,
    count_ref,
    tiles,
    a_hi,
    a_lo,
    t_hi,
    t_lo,
    turned,
    xg,
    yg,
    pbuf,
    part,
    tpart,
    drecv,
    precv,
    psum,
    zrecv,
    zsum,
    yrecv,
    small,
    ismall,
    stats,
    tile_sem,
    in_sem,
    sent_sem,
    recv_sem,
):
    z = lax.axis_index("row_0")
    yh = lax.axis_index("row_1")
    yl = lax.axis_index("col_0")
    x = lax.axis_index("col_1")
    core = lax.axis_index("col_2")
    r_me = z * 2 + yh
    c_me = (yl * 4 + x) * 2 + core

    def up4(v, d):
        return lax.rem(v + d, 4)

    def z_dev(d):
        return (up4(z, d), yh, yl, x, core)

    def x_dev(d):
        return (z, yh, yl, up4(x, d), core)

    y_far = (z, 1 - yh, yl, x, core)
    y_near = (z, yh, 1 - yl, x, core)
    other = (z, yh, yl, x, 1 - core)

    def whole(ref, sem):
        pltpu.make_async_copy(ref, ref, sem).wait()

    barrier = pltpu.get_barrier_semaphore()
    near = [z_dev(d) for d in (2, 1, 3)] + [x_dev(d) for d in (2, 1, 3)] + [y_far, y_near, other]
    near += [(z, yh, yl, up4(x, d), 1 - core) for d in (1, 3)] + [(z, yh, 1 - yl, x, 1 - core)]
    for dev in near:
        pl.semaphore_signal(barrier, inc=1, device_id=dev, device_id_type=MESH_ID)

    own_x = pl.ds(r_me * 8, 8)
    own_y = pl.ds(c_me * 8, 8)
    cp_x = pltpu.make_async_copy(primal_ref.reshape(8, 8, 128), xg.at[own_x], in_sem.at[0])
    cp_y = pltpu.make_async_copy(dual_ref.reshape(8, 8, 128), yg.at[own_y], in_sem.at[1])
    cp_x.start()
    cp_y.start()
    tables = [
        pltpu.make_async_copy(rows_hbm, tab.at[0], in_sem.at[4]),
        pltpu.make_async_copy(cols_hbm, tab.at[1], in_sem.at[4]),
        pltpu.make_async_copy(count_hbm, count_ref, in_sem.at[5]),
    ]
    for cp in tables:
        cp.start()
    cp_x.wait()
    cp_y.wait()

    def tile_copy(g):
        some = pl.ds(BATCHES[g][0], BATCHES[g][1] - BATCHES[g][0])
        return pltpu.make_async_copy(tiles_ref.at[some], tiles.at[some], tile_sem.at[g])

    for g in range(len(BATCHES)):
        tile_copy(g).start()
    mine_r = pl.ds(pl.multiple_of(c_me * 32, 32), 32)
    mine_c = pl.ds(pl.multiple_of(r_me * 32, 32), 32)
    extra = [
        pltpu.make_async_copy(req_ref.at[mine_r], small.at[0], in_sem.at[2]),
        pltpu.make_async_copy(obj_ref.at[mine_c], small.at[1], in_sem.at[2]),
        pltpu.make_async_copy(low_ref.at[mine_c], small.at[2], in_sem.at[2]),
        pltpu.make_async_copy(up_ref.at[mine_c], small.at[3], in_sem.at[2]),
        pltpu.make_async_copy(ckind_ref.at[mine_r], ismall.at[0], in_sem.at[3]),
        pltpu.make_async_copy(vkind_ref.at[mine_c], ismall.at[1], in_sem.at[3]),
    ]
    for cp in extra:
        cp.start()

    whole(tab, in_sem.at[4])
    tables[2].wait()
    lane = lax.broadcasted_iota(jnp.int32, (8, 128), 1)
    count = count_ref[0, 0]
    ridx = jnp.full((8, 128), -1, jnp.int32)
    cidx = jnp.full((8, 128), -1, jnp.int32)
    for t in range(SLOTS):
        here = (lax.rem(lane, SLOTS) == t) & (lane < 3 * SLOTS) & (jnp.full((8, 128), t, jnp.int32) < count)
        ridx = jnp.where(here, tab[0, 0, t], ridx)
        cidx = jnp.where(here, tab[1, 0, t], cidx)
    p_iota = lax.broadcasted_iota(jnp.int32, (ROW_BLOCKS, 128), 0)
    r_iota = ((p_iota // 8 % 8) * 2 + p_iota // 64) * 8 + p_iota % 8
    c_iota = lax.broadcasted_iota(jnp.int32, (COL_BLOCKS, 128), 0)
    r_hot = jnp.where(r_iota == ridx[:1], 1.0, 0.0).astype(BF16)[:, : 3 * SLOTS]
    c_hot = jnp.where(c_iota == cidx[:1], 1.0, 0.0).astype(BF16)[:, : 3 * SLOTS]

    pl.semaphore_wait(barrier, len(near))

    def send(src, dst, phase, recv, dev):
        cp = pltpu.make_async_remote_copy(
            src_ref=src,
            dst_ref=dst,
            send_sem=sent_sem.at[phase],
            recv_sem=recv if not isinstance(recv, str) else recv_sem.at[RECV.index(recv)],
            device_id=dev,
            device_id_type=MESH_ID,
        )
        cp.start()
        return cp

    def arrived(ref, name):
        whole(ref, recv_sem.at[RECV.index(name)])

    def place(g, at, recv, dev):
        send(g.at[pl.ds(at * 8, 8)], g.at[pl.ds(at * 8, 8)], 0, recv, dev)

    place(xg, r_me, "x_far", y_far)
    for d in (2, 1, 3):
        place(xg, r_me, "x_z", z_dev(d))
    place(yg, c_me, "y_n", y_near)
    place(yg, c_me, "y_x2", x_dev(2))
    for d in (1, 3):
        place(yg, c_me, "y_x", x_dev(d))
    place(yg, c_me, "y_d", other)

    def convert(g):
        tile_copy(g).wait()
        for t in range(*BATCHES[g]):
            for i in range(BLK // 128):
                sl = slice(i * 128, i * 128 + 128)
                v = tiles[t, sl, :]
                if t in VECTOR:
                    turned[VECTOR.index(t), :, sl] = v.T
                else:
                    m = MATRIX.index(t)
                    a_hi[m, sl, :], a_lo[m, sl, :] = split2(v)
                    t_hi[m, :, sl], t_lo[m, :, sl] = split2(v.T)

    for g in range(3):
        convert(g)
    arrived(yg.at[pl.ds(0, 8)], "y_n")
    at = ((1 - yl) * 4 + x) * 2 + core
    for c in (core, 1 - core):
        for d in (1, 3):
            place(yg, at, "y_d", (z, yh, yl, up4(x, d), c))
    place(yg, at, "y_d", other)
    convert(3)
    arrived(yg.at[pl.ds(0, 8)], "y_x2")
    at = (yl * 4 + up4(x, 2)) * 2 + core
    for c in (core, 1 - core):
        place(yg, at, "y_d", (z, yh, 1 - yl, x, c))
    place(yg, at, "y_d", other)
    arrived(xg.at[pl.ds(0, 8)], "x_far")
    for d in (2, 1, 3):
        place(xg, z * 2 + 1 - yh, "x_z", z_dev(d))
    arrived(yg.at[pl.ds(0, 16)], "y_x")
    for d in (1, 3):
        place(yg, (yl * 4 + up4(x, d)) * 2 + core, "y_d", other)
    convert(4)

    def scatter(hot, dest, blocks, base, rows):
        cols = []
        for e in rows:
            v = pbuf[pl.ds(e, SLOTS, stride=8), :]
            hi = v.astype(BF16)
            rest = v - hi.astype(F32)
            mid = rest.astype(BF16)
            lo = (rest - mid.astype(F32)).astype(BF16)
            cols.append(jnp.concatenate([hi, mid, lo], axis=0))
        rhs = jnp.concatenate(cols, axis=1)
        out = jnp.dot(hot, rhs, preferred_element_type=F32)
        for i in range(len(rows)):
            dest[pl.ds(base + i, blocks, stride=len(rows)), :] = out[:, i * 128 : (i + 1) * 128]

    sub = lax.broadcasted_iota(jnp.int32, (8, 128), 0)

    def vector_product(v, at, groups):
        out = jnp.zeros((8, 128), F32)
        for g in groups:
            sums = [None, None]
            for k in range(4):
                block = at(slice(g * 128, g * 128 + 128), slice(k * 128, k * 128 + 128))
                for s in range(2):
                    term = block * v[2 * k + s : 2 * k + s + 1, :]
                    sums[s] = term if sums[s] is None else sums[s] + term
            for s in range(2):
                out = jnp.where(sub == 2 * g + s, jnp.sum(sums[s].T, axis=0, keepdims=True), out)
        return out

    def products(vec, index, hi_ref, lo_ref, plain_ref, plain, groups):
        lanes = slice(groups[0] * 128, groups[-1] * 128 + 128)
        rows = slice(2 * groups[0], 2 * groups[-1] + 2)
        for t in range(SLOTS):
            v = vec[tab[index, 0, t]]
            if t in VECTOR:
                n = plain.index(t)
                out = vector_product(v, lambda r, c, n=n: plain_ref[n, r, c], groups)
            else:
                m = MATRIX.index(t)
                lhs = spread(v)
                res = jnp.dot(lhs, hi_ref[m, :, lanes], preferred_element_type=F32)
                res = res + jnp.dot(lhs, lo_ref[m, :, lanes], preferred_element_type=F32)
                out = gathered(res, groups)
            pbuf[8 * t + rows.start : 8 * t + rows.stop, :] = out[rows]

    def own_rows(zz, hh):
        return pl.ds(pl.multiple_of((zz * 2 + hh) * OWN, OWN), OWN)

    def half_rows(h, c, chip, chips=1):
        return pl.ds(pl.multiple_of(h * HALF + (c * 8 + chip) * 32, 32), chips * 32)

    arrived(yg.at[pl.ds(0, 88)], "y_d")
    products(yg, 0, a_hi, a_lo, turned, VECTOR, range(4))
    scatter(c_hot, tpart, COL_BLOCKS, 0, range(8))
    for w, hh in enumerate((1 - yh, yh)):
        for i, d in enumerate((2, 1, 3)):
            send(tpart.at[own_rows(up4(z, d), hh)], zrecv.at[w, i], 1, ("z_far", "z_near")[w], z_dev(d))
    arrived(xg.at[pl.ds(0, 48)], "x_z")
    for h in range(2):
        products(xg, 1, t_hi, t_lo, tiles, list(range(SLOTS)), range(2 * h, 2 * h + 2))
        scatter(r_hot, part, ROW_BLOCKS, h * HALF, range(4 * h, 4 * h + 4))
        send(part.at[half_rows(h, 1 - core, 0, 8)], drecv.at[h], 1, ("d_0", "d_1")[h], other)
    for h in range(2):
        arrived(drecv.at[h], ("d_0", "d_1")[h])
        mine = half_rows(h, core, 0, 8)
        part[mine, :] = part[mine, :] + drecv[h]
        for i, off in enumerate(CHIP_OFFS[:-1]):
            ny, nx = lax.rem(yl + off[0], 2), up4(x, off[1])
            send(part.at[half_rows(h, core, ny * 4 + nx)], precv.at[i, pl.ds(32 * h, 32)], 1, "p_rs", (z, yh, ny, nx, core))
    arrived(zrecv.at[0], "z_far")
    zsum[...] = tpart[own_rows(z, 1 - yh), :] + zrecv[0, 0] + zrecv[0, 1] + zrecv[0, 2]
    send(zsum, yrecv, 1, "y_rs", y_far)
    whole(small, in_sem.at[2])
    whole(ismall, in_sem.at[3])
    arrived(zrecv.at[1], "z_near")
    near_sum = tpart[own_rows(z, yh), :] + zrecv[1, 0] + zrecv[1, 1] + zrecv[1, 2]
    dual_own = [yg.reshape(ROW_BLOCKS * 8, 128)[pl.ds(c_me * OWN + s, 32, stride=2), :] for s in range(2)]
    primal_own = [xg.reshape(COL_BLOCKS * 8, 128)[pl.ds(r_me * OWN + s, 32, stride=2), :] for s in range(2)]
    stat_rows = [[], []]

    def total(v):
        return jnp.sum(v.reshape(4, 8, 128), axis=0)

    arrived(yrecv, "y_rs")
    dres_ref[...] = near_sum + yrecv[...]
    obj, low, up, vk = small[1], small[2], small[3], ismall[1]
    low_on = (vk == 1) | (vk == 3)
    up_on = (vk == 2) | (vk == 3)
    for s in range(2):
        reduced = obj - dres_ref[pl.ds(s, 32, stride=2), :]
        mult = jnp.where(low_on, jnp.maximum(reduced, 0.0), 0.0) + jnp.where(
            up_on, jnp.minimum(reduced, 0.0), 0.0
        )
        res = reduced - mult
        dres_ref[pl.ds(s, 32, stride=2), :] = res
        bound = low * jnp.maximum(mult, 0.0) + up * jnp.minimum(mult, 0.0)
        stat_rows[s] += [
            total(res * res),
            total(obj * obj),
            total(obj * primal_own[s]),
            total(bound),
        ]
    arrived(precv, "p_rs")
    for h in range(2):
        product = part[half_rows(h, core, yl * 4 + x), :]
        for i in range(7):
            product = product + precv[i, 32 * h : 32 * h + 32, :]
        psum[32 * h : 32 * h + 32, :] = product
    for h in range(2):
        for e in range(4):
            pres_ref[pl.ds(4 * h + e, 8, stride=8), :] = psum[pl.ds(32 * h + e, 8, stride=4), :]
    req = small[0]
    is_ge = ismall[0] == 1
    for s in range(2):
        diff = req - pres_ref[pl.ds(s, 32, stride=2), :]
        res = jnp.where(is_ge, jnp.maximum(diff, 0.0), diff)
        pres_ref[pl.ds(s, 32, stride=2), :] = res
        stat_rows[s] += [total(res * res), total(req * req), total(req * dual_own[s])]

    lane1 = lax.broadcasted_iota(jnp.int32, (1, 128), 1)
    acc = jnp.zeros((1, 128), F32)
    for s in range(2):
        for q in range(7):
            v = jnp.sum(stat_rows[s][q], axis=0, keepdims=True)
            v = jnp.sum(v, axis=1, keepdims=True)
            acc = jnp.where(lane1 == 7 * s + q, v, acc)
    me = r_me * 16 + c_me
    stats[me] = acc
    for dz, dh, dl, dx, dc in PEERS:
        dev = (up4(z, dz), lax.rem(yh + dh, 2), lax.rem(yl + dl, 2), up4(x, dx), lax.rem(core + dc, 2))
        send(stats.at[me], stats.at[me], 2, "stat", dev)
    arrived(stats.at[pl.ds(0, 127)], "stat")
    acc = jnp.sum(stats[...], axis=0)

    pick = [jnp.concatenate([acc[:, q : q + 1], acc[:, 7 + q : 8 + q]], axis=0) for q in range(7)]
    primal_square, require_square, require_dot = pick[4], pick[5], pick[6]
    dual_square, objective_square, objective_dot, bound_sum = pick[0], pick[1], pick[2], pick[3]
    primal_ratio = jnp.sqrt(primal_square) / (1.0 + jnp.sqrt(require_square))
    dual_ratio = jnp.sqrt(dual_square) / (1.0 + jnp.sqrt(objective_square))
    dual_value = require_dot + bound_sum
    gap = jnp.abs(objective_dot - dual_value) / (1.0 + jnp.abs(objective_dot) + jnp.abs(dual_value))
    lane2 = lax.broadcasted_iota(jnp.int32, (2, 128), 1)
    met = jnp.where(lane2 == 0, primal_ratio, jnp.where(lane2 == 1, dual_ratio, gap))
    met_ref[...] = met[:, :3]

    whole(tiles.at[0, pl.ds(0, 352)], sent_sem.at[0])
    whole(tiles.at[0, pl.ds(0, 352)], sent_sem.at[1])
    whole(stats.at[pl.ds(0, 127)], sent_sem.at[2])


def flush(a, b, c, a_out, b_out, c_out, sem):
    copies = [
        pltpu.make_async_copy(src, dst, sem.at[i])
        for i, (src, dst) in enumerate(((a, a_out), (b, b_out), (c, c_out)))
    ]
    for cp in copies:
        cp.start()
    for cp in copies:
        cp.wait()


def interleave(a):
    return a.reshape(2, 32, 128).transpose(1, 0, 2).reshape(OWN, 128)


def deinterleave(a):
    return a.reshape(32, 2, 128).transpose(1, 0, 2).reshape(2, 4096)


def on_device(
    matrix_tiles,
    tile_rows,
    tile_columns,
    tile_counts,
    primal_iter,
    dual_iter,
    requirement,
    constraint_kind,
    objective,
    lower_bound,
    upper_bound,
    variable_kind,
):
    hbm = pl.BlockSpec(memory_space=pl.ANY)
    vmem = pl.BlockSpec(memory_space=pltpu.VMEM)
    dma = pltpu.SemaphoreType.DMA
    pres, dres, metrics = pl.pallas_call(
        kernel,
        name="restart_check",
        out_shape=(
            pltpu.VMEM((OWN, 128), F32),
            pltpu.VMEM((OWN, 128), F32),
            pltpu.VMEM((2, 3), F32),
        ),
        in_specs=[hbm] * 12,
        out_specs=(vmem, vmem, vmem),
        scratch_shapes=[
            pltpu.SMEM((2, 1, SLOTS), jnp.int32),
            pltpu.SMEM((1, 1), jnp.int32),
            pltpu.VMEM((SLOTS, BLK, BLK), F32),
            pltpu.VMEM((len(MATRIX), BLK, BLK), BF16),
            pltpu.VMEM((len(MATRIX), BLK, BLK), BF16),
            pltpu.VMEM((len(MATRIX), BLK, BLK), BF16),
            pltpu.VMEM((len(MATRIX), BLK, BLK), BF16),
            pltpu.VMEM((len(VECTOR), BLK, BLK), F32),
            pltpu.VMEM((COL_BLOCKS, 8, 128), F32),
            pltpu.VMEM((ROW_BLOCKS, 8, 128), F32),
            pltpu.VMEM((SLOTS * 8, 128), F32),
            pltpu.VMEM((16 * OWN, 128), F32),
            pltpu.VMEM((8 * OWN, 128), F32),
            pltpu.VMEM((2, HALF // 2, 128), F32),
            pltpu.VMEM((7, OWN, 128), F32),
            pltpu.VMEM((OWN, 128), F32),
            pltpu.VMEM((2, 3, OWN, 128), F32),
            pltpu.VMEM((OWN, 128), F32),
            pltpu.VMEM((OWN, 128), F32),
            pltpu.VMEM((4, 32, 128), F32),
            pltpu.VMEM((2, 32, 128), jnp.int32),
            pltpu.VMEM((128, 1, 128), F32),
            dma((len(BATCHES),)),
            dma((6,)),
            dma((3,)),
            dma((len(RECV),)),
        ],
        compiler_params=pltpu.CompilerParams(
            collective_id=0, has_side_effects=True, vmem_limit_bytes=60 * 1024 * 1024
        ),
    )(
        tile_rows.reshape(1, SLOTS),
        tile_columns.reshape(1, SLOTS),
        tile_counts,
        matrix_tiles.reshape(SLOTS, BLK, BLK),
        interleave(primal_iter),
        interleave(dual_iter),
        requirement.reshape(512, 128),
        constraint_kind.reshape(512, 128),
        objective.reshape(256, 128),
        lower_bound.reshape(256, 128),
        upper_bound.reshape(256, 128),
        variable_kind.reshape(256, 128),
    )
    pres, dres, metrics = pl.pallas_call(
        flush,
        name="flush",
        out_shape=(
            pltpu.HBM((OWN, 128), F32),
            pltpu.HBM((OWN, 128), F32),
            pltpu.HBM((2, 3), F32),
        ),
        in_specs=[vmem] * 3,
        out_specs=(hbm,) * 3,
        scratch_shapes=[dma((3,))],
        compiler_params=pltpu.CompilerParams(vmem_limit_bytes=1024 * 1024),
    )(pres, dres, metrics)
    return deinterleave(pres), deinterleave(dres), metrics


def solution(mesh):
    torus = Mesh(mesh.devices.reshape(4, 2, 2, 4, 2), ROW_COL)
    return jax.shard_map(
        on_device,
        mesh=torus,
        in_specs=(
            P(ROW, COL, None, None, None),
            P(ROW, COL, None),
            P(ROW, COL, None),
            P(ROW, COL),
            P(None, COL_ROW),
            P(None, ROW_COL),
            P(ROW),
            P(ROW),
            P(COL),
            P(COL),
            P(COL),
            P(COL),
        ),
        out_specs=(P(None, ROW_COL), P(None, COL_ROW), P()),
        check_vma=False,
    )
```

```python
import jax
import jax.numpy as jnp
from jax import lax
from jax.experimental import pallas as pl
from jax.experimental.pallas import tpu as pltpu
from jax.sharding import Mesh
from jax.sharding import PartitionSpec as P

ROW = ("row_0", "row_1")
COL = ("col_0", "col_1", "col_2")
ROW_COL = ROW + COL
COL_ROW = COL + ROW
MESH_ID = pl.DeviceIdType.MESH

BLK = 512
SLOTS = 16
ROW_BLOCKS = 128
COL_BLOCKS = 64
HALF = 512
OWN = 64

CHIP_OFFS = [(1, 2), (1, 1), (1, 3), (0, 2), (1, 0), (0, 1), (0, 3), (0, 0)]
VECTOR = [1, 3, 5, 7, 9, 11, 13, 15]
MATRIX = [t for t in range(SLOTS) if t not in VECTOR]
BATCHES = [(0, 3), (3, 6), (6, 9), (9, 12), (12, 16)]
RECV = ["x_far", "x_z", "y_n", "y_x", "y_x2", "y_d", "d_0", "d_1", "z_far", "z_near", "y_rs", "p_rs", "stat"]


def hops(off):
    dz, dh, dl, dx, dc = off
    return min(dz, 4 - dz) + min(dx, 4 - dx) + (2 * dh if not dl else 1) + 0.2 * dc


PEERS = [
    (dz, dh, dl, dx, dc)
    for dz in range(4)
    for dh in range(2)
    for dl in range(2)
    for dx in range(4)
    for dc in range(2)
]
PEERS = sorted(PEERS[1:], key=hops, reverse=True)
F32 = jnp.float32
BF16 = jnp.bfloat16


def split2(v):
    hi = v.astype(BF16)
    lo = (v - hi.astype(F32)).astype(BF16)
    return hi, lo


def spread(v):
    sub = lax.broadcasted_iota(jnp.int32, (8, 128), 0)
    hi = v.astype(BF16).astype(F32)
    lo = v - hi
    parts = []
    for k in range(4):
        keep = (sub // 2) == k
        parts.append(jnp.concatenate([jnp.where(keep, hi, 0.0), jnp.where(keep, lo, 0.0)], axis=0))
    return jnp.concatenate(parts, axis=1).astype(BF16)


def gathered(r, groups):
    sub = lax.broadcasted_iota(jnp.int32, (8, 128), 0)
    out = jnp.zeros((8, 128), F32)
    for i, g in enumerate(groups):
        c = r[:8, 128 * i : 128 * i + 128] + r[8:, 128 * i : 128 * i + 128]
        c = c + pltpu.roll(c, 2, 0)
        c = c + pltpu.roll(c, 4, 0)
        out = jnp.where((sub // 2) == g, c, out)
    return out


def kernel(
    rows_hbm,
    cols_hbm,
    count_hbm,
    tiles_ref,
    primal_ref,
    dual_ref,
    req_ref,
    ckind_ref,
    obj_ref,
    low_ref,
    up_ref,
    vkind_ref,
    pres_ref,
    dres_ref,
    met_ref,
    tab,
    count_ref,
    tiles,
    a_hi,
    a_lo,
    t_hi,
    t_lo,
    turned,
    xg,
    yg,
    pbuf,
    part,
    tpart,
    drecv,
    precv,
    psum,
    zrecv,
    zsum,
    yrecv,
    small,
    ismall,
    stats,
    tile_sem,
    in_sem,
    sent_sem,
    recv_sem,
):
    z = lax.axis_index("row_0")
    yh = lax.axis_index("row_1")
    yl = lax.axis_index("col_0")
    x = lax.axis_index("col_1")
    core = lax.axis_index("col_2")
    r_me = z * 2 + yh
    c_me = (yl * 4 + x) * 2 + core

    def up4(v, d):
        return lax.rem(v + d, 4)

    def z_dev(d):
        return (up4(z, d), yh, yl, x, core)

    def x_dev(d):
        return (z, yh, yl, up4(x, d), core)

    y_far = (z, 1 - yh, yl, x, core)
    y_near = (z, yh, 1 - yl, x, core)
    other = (z, yh, yl, x, 1 - core)

    def whole(ref, sem):
        pltpu.make_async_copy(ref, ref, sem).wait()

    barrier = pltpu.get_barrier_semaphore()
    near = [z_dev(d) for d in (2, 1, 3)] + [x_dev(d) for d in (2, 1, 3)] + [y_far, y_near, other]
    near += [(z, yh, yl, up4(x, d), 1 - core) for d in (1, 3)] + [(z, yh, 1 - yl, x, 1 - core)]
    for dev in near:
        pl.semaphore_signal(barrier, inc=1, device_id=dev, device_id_type=MESH_ID)

    own_x = pl.ds(r_me * 8, 8)
    own_y = pl.ds(c_me * 8, 8)
    cp_x = pltpu.make_async_copy(primal_ref.reshape(8, 8, 128), xg.at[own_x], in_sem.at[0])
    cp_y = pltpu.make_async_copy(dual_ref.reshape(8, 8, 128), yg.at[own_y], in_sem.at[1])
    cp_x.start()
    cp_y.start()
    tables = [
        pltpu.make_async_copy(rows_hbm, tab.at[0], in_sem.at[4]),
        pltpu.make_async_copy(cols_hbm, tab.at[1], in_sem.at[4]),
        pltpu.make_async_copy(count_hbm, count_ref, in_sem.at[5]),
    ]
    for cp in tables:
        cp.start()
    cp_x.wait()
    cp_y.wait()

    def tile_copy(g):
        some = pl.ds(BATCHES[g][0], BATCHES[g][1] - BATCHES[g][0])
        return pltpu.make_async_copy(tiles_ref.at[some], tiles.at[some], tile_sem.at[g])

    for g in range(len(BATCHES)):
        tile_copy(g).start()
    mine_r = pl.ds(pl.multiple_of(c_me * 32, 32), 32)
    mine_c = pl.ds(pl.multiple_of(r_me * 32, 32), 32)
    extra = [
        pltpu.make_async_copy(req_ref.at[mine_r], small.at[0], in_sem.at[2]),
        pltpu.make_async_copy(obj_ref.at[mine_c], small.at[1], in_sem.at[2]),
        pltpu.make_async_copy(low_ref.at[mine_c], small.at[2], in_sem.at[2]),
        pltpu.make_async_copy(up_ref.at[mine_c], small.at[3], in_sem.at[2]),
        pltpu.make_async_copy(ckind_ref.at[mine_r], ismall.at[0], in_sem.at[3]),
        pltpu.make_async_copy(vkind_ref.at[mine_c], ismall.at[1], in_sem.at[3]),
    ]
    for cp in extra:
        cp.start()

    whole(tab, in_sem.at[4])
    tables[2].wait()
    lane = lax.broadcasted_iota(jnp.int32, (8, 128), 1)
    count = count_ref[0, 0]
    ridx = jnp.full((8, 128), -1, jnp.int32)
    cidx = jnp.full((8, 128), -1, jnp.int32)
    for t in range(SLOTS):
        here = (lax.rem(lane, SLOTS) == t) & (lane < 3 * SLOTS) & (jnp.full((8, 128), t, jnp.int32) < count)
        ridx = jnp.where(here, tab[0, 0, t], ridx)
        cidx = jnp.where(here, tab[1, 0, t], cidx)
    p_iota = lax.broadcasted_iota(jnp.int32, (ROW_BLOCKS, 128), 0)
    r_iota = ((p_iota // 8 % 8) * 2 + p_iota // 64) * 8 + p_iota % 8
    c_iota = lax.broadcasted_iota(jnp.int32, (COL_BLOCKS, 128), 0)
    r_hot = jnp.where(r_iota == ridx[:1], 1.0, 0.0).astype(BF16)[:, : 3 * SLOTS]
    c_hot = jnp.where(c_iota == cidx[:1], 1.0, 0.0).astype(BF16)[:, : 3 * SLOTS]

    pl.semaphore_wait(barrier, len(near))

    def send(src, dst, phase, recv, dev):
        cp = pltpu.make_async_remote_copy(
            src_ref=src,
            dst_ref=dst,
            send_sem=sent_sem.at[phase],
            recv_sem=recv if not isinstance(recv, str) else recv_sem.at[RECV.index(recv)],
            device_id=dev,
            device_id_type=MESH_ID,
        )
        cp.start()
        return cp

    def arrived(ref, name):
        whole(ref, recv_sem.at[RECV.index(name)])

    def place(g, at, recv, dev):
        send(g.at[pl.ds(at * 8, 8)], g.at[pl.ds(at * 8, 8)], 0, recv, dev)

    place(yg, c_me, "y_n", y_near)
    place(xg, r_me, "x_far", y_far)
    place(yg, c_me, "y_x2", x_dev(2))
    for d in (2, 1, 3):
        place(xg, r_me, "x_z", z_dev(d))
    for d in (1, 3):
        place(yg, c_me, "y_x", x_dev(d))
    place(yg, c_me, "y_d", other)

    def convert(*which):
        for t in which:
            for g, (begin, _) in enumerate(BATCHES):
                if t == begin:
                    tile_copy(g).wait()
            for i in range(BLK // 128):
                sl = slice(i * 128, i * 128 + 128)
                v = tiles[t, sl, :]
                if t in VECTOR:
                    turned[VECTOR.index(t), :, sl] = v.T
                else:
                    m = MATRIX.index(t)
                    a_hi[m, sl, :], a_lo[m, sl, :] = split2(v)
                    t_hi[m, :, sl], t_lo[m, :, sl] = split2(v.T)

    convert(*range(6))
    arrived(yg.at[pl.ds(0, 8)], "y_n")
    at = ((1 - yl) * 4 + x) * 2 + core
    for c in (core, 1 - core):
        for d in (1, 3):
            place(yg, at, "y_d", (z, yh, yl, up4(x, d), c))
    place(yg, at, "y_d", other)
    convert(6, 7, 8)
    arrived(yg.at[pl.ds(0, 8)], "y_x2")
    at = (yl * 4 + up4(x, 2)) * 2 + core
    for c in (core, 1 - core):
        place(yg, at, "y_d", (z, yh, 1 - yl, x, c))
    place(yg, at, "y_d", other)
    convert(9)
    arrived(xg.at[pl.ds(0, 8)], "x_far")
    for d in (2, 1, 3):
        place(xg, z * 2 + 1 - yh, "x_z", z_dev(d))
    arrived(yg.at[pl.ds(0, 16)], "y_x")
    for d in (1, 3):
        place(yg, (yl * 4 + up4(x, d)) * 2 + core, "y_d", other)
    convert(*range(10, SLOTS))

    def scatter(hot, dest, blocks, base, rows):
        cols = []
        for e in rows:
            v = pbuf[pl.ds(e, SLOTS, stride=8), :]
            hi = v.astype(BF16)
            rest = v - hi.astype(F32)
            mid = rest.astype(BF16)
            lo = (rest - mid.astype(F32)).astype(BF16)
            cols.append(jnp.concatenate([hi, mid, lo], axis=0))
        rhs = jnp.concatenate(cols, axis=1)
        out = jnp.dot(hot, rhs, preferred_element_type=F32)
        for i in range(len(rows)):
            dest[pl.ds(base + i, blocks, stride=len(rows)), :] = out[:, i * 128 : (i + 1) * 128]

    sub = lax.broadcasted_iota(jnp.int32, (8, 128), 0)

    def vector_product(v, at, groups):
        out = jnp.zeros((8, 128), F32)
        for g in groups:
            sums = [None, None]
            for k in range(4):
                block = at(slice(g * 128, g * 128 + 128), slice(k * 128, k * 128 + 128))
                for s in range(2):
                    term = block * v[2 * k + s : 2 * k + s + 1, :]
                    sums[s] = term if sums[s] is None else sums[s] + term
            for s in range(2):
                out = jnp.where(sub == 2 * g + s, jnp.sum(sums[s].T, axis=0, keepdims=True), out)
        return out

    def products(vec, index, hi_ref, lo_ref, plain_ref, plain, groups):
        lanes = slice(groups[0] * 128, groups[-1] * 128 + 128)
        rows = slice(2 * groups[0], 2 * groups[-1] + 2)
        for t in range(SLOTS):
            v = vec[tab[index, 0, t]]
            if t in VECTOR:
                n = plain.index(t)
                out = vector_product(v, lambda r, c, n=n: plain_ref[n, r, c], groups)
            else:
                m = MATRIX.index(t)
                lhs = spread(v)
                res = jnp.dot(lhs, hi_ref[m, :, lanes], preferred_element_type=F32)
                res = res + jnp.dot(lhs, lo_ref[m, :, lanes], preferred_element_type=F32)
                out = gathered(res, groups)
            pbuf[8 * t + rows.start : 8 * t + rows.stop, :] = out[rows]

    def own_rows(zz, hh):
        return pl.ds(pl.multiple_of((zz * 2 + hh) * OWN, OWN), OWN)

    def half_rows(h, c, chip, chips=1):
        return pl.ds(pl.multiple_of(h * HALF + (c * 8 + chip) * 32, 32), chips * 32)

    arrived(yg.at[pl.ds(0, 88)], "y_d")
    products(yg, 0, a_hi, a_lo, turned, VECTOR, range(4))
    scatter(c_hot, tpart, COL_BLOCKS, 0, range(8))
    for w, hh in enumerate((1 - yh, yh)):
        for i, d in enumerate((2, 1, 3)):
            send(tpart.at[own_rows(up4(z, d), hh)], zrecv.at[w, i], 1, ("z_far", "z_near")[w], z_dev(d))
    arrived(xg.at[pl.ds(0, 48)], "x_z")
    for h in range(2):
        products(xg, 1, t_hi, t_lo, tiles, list(range(SLOTS)), range(2 * h, 2 * h + 2))
        scatter(r_hot, part, ROW_BLOCKS, h * HALF, range(4 * h, 4 * h + 4))
        send(part.at[half_rows(h, 1 - core, 0, 8)], drecv.at[h], 1, ("d_0", "d_1")[h], other)
    def hand_out(h, steps):
        for i, off in enumerate(CHIP_OFFS[:-1]):
            if off[0] in steps:
                ny, nx = lax.rem(yl + off[0], 2), up4(x, off[1])
                dev = (z, yh, ny, nx, core)
                send(part.at[half_rows(h, core, ny * 4 + nx)], precv.at[i, pl.ds(32 * h, 32)], 1, "p_rs", dev)

    for h in range(2):
        arrived(drecv.at[h], ("d_0", "d_1")[h])
        mine = half_rows(h, core, 0, 8)
        part[mine, :] = part[mine, :] + drecv[h]
        hand_out(h, (0, 1) if h == 0 else (0,))
    arrived(zrecv.at[0], "z_far")
    zsum[...] = tpart[own_rows(z, 1 - yh), :] + zrecv[0, 0] + zrecv[0, 1] + zrecv[0, 2]
    send(zsum, yrecv, 1, "y_rs", y_far)
    hand_out(1, (1,))
    whole(small, in_sem.at[2])
    whole(ismall, in_sem.at[3])
    arrived(zrecv.at[1], "z_near")
    near_sum = tpart[own_rows(z, yh), :] + zrecv[1, 0] + zrecv[1, 1] + zrecv[1, 2]
    dual_own = [yg.reshape(ROW_BLOCKS * 8, 128)[pl.ds(c_me * OWN + s, 32, stride=2), :] for s in range(2)]
    primal_own = [xg.reshape(COL_BLOCKS * 8, 128)[pl.ds(r_me * OWN + s, 32, stride=2), :] for s in range(2)]
    stat_rows = [[], []]

    def total(v):
        return jnp.sum(v.reshape(4, 8, 128), axis=0)

    lane1 = lax.broadcasted_iota(jnp.int32, (1, 128), 1)

    def lane_sums(acc, begin, end):
        for s in range(2):
            for q in range(begin, end):
                v = jnp.sum(stat_rows[s][q], axis=0, keepdims=True)
                v = jnp.sum(v, axis=1, keepdims=True)
                acc = jnp.where(lane1 == 7 * s + q, v, acc)
        return acc

    arrived(yrecv, "y_rs")
    dres_ref[...] = near_sum + yrecv[...]
    obj, low, up, vk = small[1], small[2], small[3], ismall[1]
    low_on = (vk == 1) | (vk == 3)
    up_on = (vk == 2) | (vk == 3)
    for s in range(2):
        reduced = obj - dres_ref[pl.ds(s, 32, stride=2), :]
        mult = jnp.where(low_on, jnp.maximum(reduced, 0.0), 0.0) + jnp.where(
            up_on, jnp.minimum(reduced, 0.0), 0.0
        )
        res = reduced - mult
        dres_ref[pl.ds(s, 32, stride=2), :] = res
        bound = low * jnp.maximum(mult, 0.0) + up * jnp.minimum(mult, 0.0)
        stat_rows[s] += [
            total(res * res),
            total(obj * obj),
            total(obj * primal_own[s]),
            total(bound),
        ]
    acc = lane_sums(jnp.zeros((1, 128), F32), 0, 4)
    arrived(precv, "p_rs")
    for h in range(2):
        product = part[half_rows(h, core, yl * 4 + x), :]
        for i in range(7):
            product = product + precv[i, 32 * h : 32 * h + 32, :]
        psum[32 * h : 32 * h + 32, :] = product
    for h in range(2):
        for e in range(4):
            pres_ref[pl.ds(4 * h + e, 8, stride=8), :] = psum[pl.ds(32 * h + e, 8, stride=4), :]
    req = small[0]
    is_ge = ismall[0] == 1
    for s in range(2):
        diff = req - pres_ref[pl.ds(s, 32, stride=2), :]
        res = jnp.where(is_ge, jnp.maximum(diff, 0.0), diff)
        pres_ref[pl.ds(s, 32, stride=2), :] = res
        stat_rows[s] += [total(res * res), total(req * req), total(req * dual_own[s])]

    me = r_me * 16 + c_me
    stats[me] = lane_sums(acc, 4, 7)
    for dz, dh, dl, dx, dc in PEERS:
        dev = (up4(z, dz), lax.rem(yh + dh, 2), lax.rem(yl + dl, 2), up4(x, dx), lax.rem(core + dc, 2))
        send(stats.at[me], stats.at[me], 2, "stat", dev)
    arrived(stats.at[pl.ds(0, 127)], "stat")
    acc = jnp.sum(stats[...], axis=0)

    pick = [jnp.concatenate([acc[:, q : q + 1], acc[:, 7 + q : 8 + q]], axis=0) for q in range(7)]
    primal_square, require_square, require_dot = pick[4], pick[5], pick[6]
    dual_square, objective_square, objective_dot, bound_sum = pick[0], pick[1], pick[2], pick[3]
    primal_ratio = jnp.sqrt(primal_square) / (1.0 + jnp.sqrt(require_square))
    dual_ratio = jnp.sqrt(dual_square) / (1.0 + jnp.sqrt(objective_square))
    dual_value = require_dot + bound_sum
    gap = jnp.abs(objective_dot - dual_value) / (1.0 + jnp.abs(objective_dot) + jnp.abs(dual_value))
    lane2 = lax.broadcasted_iota(jnp.int32, (2, 128), 1)
    met = jnp.where(lane2 == 0, primal_ratio, jnp.where(lane2 == 1, dual_ratio, gap))
    met_ref[...] = met[:, :3]

    whole(tiles.at[0, pl.ds(0, 352)], sent_sem.at[0])
    whole(tiles.at[0, pl.ds(0, 352)], sent_sem.at[1])
    whole(stats.at[pl.ds(0, 127)], sent_sem.at[2])


def flush(a, b, c, a_out, b_out, c_out, sem):
    copies = [
        pltpu.make_async_copy(src, dst, sem.at[i])
        for i, (src, dst) in enumerate(((a, a_out), (b, b_out), (c, c_out)))
    ]
    for cp in copies:
        cp.start()
    for cp in copies:
        cp.wait()


def interleave(a):
    return a.reshape(2, 32, 128).transpose(1, 0, 2).reshape(OWN, 128)


def deinterleave(a):
    return a.reshape(32, 2, 128).transpose(1, 0, 2).reshape(2, 4096)


def on_device(
    matrix_tiles,
    tile_rows,
    tile_columns,
    tile_counts,
    primal_iter,
    dual_iter,
    requirement,
    constraint_kind,
    objective,
    lower_bound,
    upper_bound,
    variable_kind,
):
    hbm = pl.BlockSpec(memory_space=pl.ANY)
    vmem = pl.BlockSpec(memory_space=pltpu.VMEM)
    dma = pltpu.SemaphoreType.DMA
    pres, dres, metrics = pl.pallas_call(
        kernel,
        name="restart_check",
        out_shape=(
            pltpu.VMEM((OWN, 128), F32),
            pltpu.VMEM((OWN, 128), F32),
            pltpu.VMEM((2, 3), F32),
        ),
        in_specs=[hbm] * 12,
        out_specs=(vmem, vmem, vmem),
        scratch_shapes=[
            pltpu.SMEM((2, 1, SLOTS), jnp.int32),
            pltpu.SMEM((1, 1), jnp.int32),
            pltpu.VMEM((SLOTS, BLK, BLK), F32),
            pltpu.VMEM((len(MATRIX), BLK, BLK), BF16),
            pltpu.VMEM((len(MATRIX), BLK, BLK), BF16),
            pltpu.VMEM((len(MATRIX), BLK, BLK), BF16),
            pltpu.VMEM((len(MATRIX), BLK, BLK), BF16),
            pltpu.VMEM((len(VECTOR), BLK, BLK), F32),
            pltpu.VMEM((COL_BLOCKS, 8, 128), F32),
            pltpu.VMEM((ROW_BLOCKS, 8, 128), F32),
            pltpu.VMEM((SLOTS * 8, 128), F32),
            pltpu.VMEM((16 * OWN, 128), F32),
            pltpu.VMEM((8 * OWN, 128), F32),
            pltpu.VMEM((2, HALF // 2, 128), F32),
            pltpu.VMEM((7, OWN, 128), F32),
            pltpu.VMEM((OWN, 128), F32),
            pltpu.VMEM((2, 3, OWN, 128), F32),
            pltpu.VMEM((OWN, 128), F32),
            pltpu.VMEM((OWN, 128), F32),
            pltpu.VMEM((4, 32, 128), F32),
            pltpu.VMEM((2, 32, 128), jnp.int32),
            pltpu.VMEM((128, 1, 128), F32),
            dma((len(BATCHES),)),
            dma((6,)),
            dma((3,)),
            dma((len(RECV),)),
        ],
        compiler_params=pltpu.CompilerParams(
            collective_id=0, has_side_effects=True, vmem_limit_bytes=60 * 1024 * 1024
        ),
    )(
        tile_rows.reshape(1, SLOTS),
        tile_columns.reshape(1, SLOTS),
        tile_counts,
        matrix_tiles.reshape(SLOTS, BLK, BLK),
        interleave(primal_iter),
        interleave(dual_iter),
        requirement.reshape(512, 128),
        constraint_kind.reshape(512, 128),
        objective.reshape(256, 128),
        lower_bound.reshape(256, 128),
        upper_bound.reshape(256, 128),
        variable_kind.reshape(256, 128),
    )
    pres, dres, metrics = pl.pallas_call(
        flush,
        name="flush",
        out_shape=(
            pltpu.HBM((OWN, 128), F32),
            pltpu.HBM((OWN, 128), F32),
            pltpu.HBM((2, 3), F32),
        ),
        in_specs=[vmem] * 3,
        out_specs=(hbm,) * 3,
        scratch_shapes=[dma((3,))],
        compiler_params=pltpu.CompilerParams(vmem_limit_bytes=1024 * 1024),
    )(pres, dres, metrics)
    return deinterleave(pres), deinterleave(dres), metrics


def solution(mesh):
    torus = Mesh(mesh.devices.reshape(4, 2, 2, 4, 2), ROW_COL)
    return jax.shard_map(
        on_device,
        mesh=torus,
        in_specs=(
            P(ROW, COL, None, None, None),
            P(ROW, COL, None),
            P(ROW, COL, None),
            P(ROW, COL),
            P(None, COL_ROW),
            P(None, ROW_COL),
            P(ROW),
            P(ROW),
            P(COL),
            P(COL),
            P(COL),
            P(COL),
        ),
        out_specs=(P(None, ROW_COL), P(None, COL_ROW), P()),
        check_vma=False,
    )
```

```python
import jax
import jax.numpy as jnp
from jax import lax
from jax.experimental import pallas as pl
from jax.experimental.pallas import tpu as pltpu
from jax.sharding import Mesh
from jax.sharding import PartitionSpec as P

ROW = ("row_0", "row_1")
COL = ("col_0", "col_1", "col_2")
ROW_COL = ROW + COL
COL_ROW = COL + ROW
MESH_ID = pl.DeviceIdType.MESH

BLK = 512
SLOTS = 16
ROW_BLOCKS = 128
COL_BLOCKS = 64
HALF = 512
OWN = 64

CHIP_OFFS = [(1, 2), (1, 1), (1, 3), (0, 2), (1, 0), (0, 1), (0, 3), (0, 0)]
VECTOR = [1, 3, 5, 7, 9, 11, 13, 15]
MATRIX = [t for t in range(SLOTS) if t not in VECTOR]
BATCHES = [(0, 3), (3, 6), (6, 9), (9, 12), (12, 16)]
RECV = ["x_far", "x_z", "y_n", "y_x", "y_x2", "y_d", "d_0", "d_1", "z_far", "z_near", "y_rs", "p_rs", "stat"]


def hops(off):
    dz, dh, dl, dx, dc = off
    return min(dz, 4 - dz) + min(dx, 4 - dx) + (2 * dh if not dl else 1) + 0.2 * dc


PEERS = [
    (dz, dh, dl, dx, dc)
    for dz in range(4)
    for dh in range(2)
    for dl in range(2)
    for dx in range(4)
    for dc in range(2)
]
PEERS = sorted(PEERS[1:], key=hops, reverse=True)
F32 = jnp.float32
BF16 = jnp.bfloat16


def split2(v):
    hi = v.astype(BF16)
    lo = (v - hi.astype(F32)).astype(BF16)
    return hi, lo


def spread(v):
    sub = lax.broadcasted_iota(jnp.int32, (8, 128), 0)
    hi = v.astype(BF16).astype(F32)
    lo = v - hi
    parts = []
    for k in range(4):
        keep = (sub // 2) == k
        parts.append(jnp.concatenate([jnp.where(keep, hi, 0.0), jnp.where(keep, lo, 0.0)], axis=0))
    return jnp.concatenate(parts, axis=1).astype(BF16)


def gathered(r, groups):
    sub = lax.broadcasted_iota(jnp.int32, (8, 128), 0)
    out = jnp.zeros((8, 128), F32)
    for i, g in enumerate(groups):
        c = r[:8, 128 * i : 128 * i + 128] + r[8:, 128 * i : 128 * i + 128]
        c = c + pltpu.roll(c, 2, 0)
        c = c + pltpu.roll(c, 4, 0)
        out = jnp.where((sub // 2) == g, c, out)
    return out


def kernel(
    rows_hbm,
    cols_hbm,
    count_hbm,
    tiles_ref,
    primal_ref,
    dual_ref,
    req_ref,
    ckind_ref,
    obj_ref,
    low_ref,
    up_ref,
    vkind_ref,
    pres_ref,
    dres_ref,
    met_ref,
    tab,
    count_ref,
    tiles,
    a_hi,
    a_lo,
    t_hi,
    t_lo,
    turned,
    xg,
    yg,
    pbuf,
    part,
    tpart,
    drecv,
    precv,
    psum,
    zrecv,
    zsum,
    yrecv,
    small,
    ismall,
    stats,
    tile_sem,
    in_sem,
    sent_sem,
    recv_sem,
):
    z = lax.axis_index("row_0")
    yh = lax.axis_index("row_1")
    yl = lax.axis_index("col_0")
    x = lax.axis_index("col_1")
    core = lax.axis_index("col_2")
    r_me = z * 2 + yh
    c_me = (yl * 4 + x) * 2 + core

    def up4(v, d):
        return lax.rem(v + d, 4)

    def z_dev(d):
        return (up4(z, d), yh, yl, x, core)

    def x_dev(d):
        return (z, yh, yl, up4(x, d), core)

    y_far = (z, 1 - yh, yl, x, core)
    y_near = (z, yh, 1 - yl, x, core)
    other = (z, yh, yl, x, 1 - core)

    def whole(ref, sem):
        pltpu.make_async_copy(ref, ref, sem).wait()

    barrier = pltpu.get_barrier_semaphore()
    near = [z_dev(d) for d in (2, 1, 3)] + [x_dev(d) for d in (2, 1, 3)] + [y_far, y_near, other]
    near += [(z, yh, yl, up4(x, d), 1 - core) for d in (1, 3)] + [(z, yh, 1 - yl, x, 1 - core)]
    for dev in near:
        pl.semaphore_signal(barrier, inc=1, device_id=dev, device_id_type=MESH_ID)

    own_x = pl.ds(r_me * 8, 8)
    own_y = pl.ds(c_me * 8, 8)
    cp_x = pltpu.make_async_copy(primal_ref.reshape(8, 8, 128), xg.at[own_x], in_sem.at[0])
    cp_y = pltpu.make_async_copy(dual_ref.reshape(8, 8, 128), yg.at[own_y], in_sem.at[1])
    cp_x.start()
    cp_y.start()
    tables = [
        pltpu.make_async_copy(rows_hbm, tab.at[0], in_sem.at[4]),
        pltpu.make_async_copy(cols_hbm, tab.at[1], in_sem.at[4]),
        pltpu.make_async_copy(count_hbm, count_ref, in_sem.at[5]),
    ]
    for cp in tables:
        cp.start()
    cp_x.wait()
    cp_y.wait()

    def tile_copy(g):
        some = pl.ds(BATCHES[g][0], BATCHES[g][1] - BATCHES[g][0])
        return pltpu.make_async_copy(tiles_ref.at[some], tiles.at[some], tile_sem.at[g])

    for g in range(len(BATCHES)):
        tile_copy(g).start()
    mine_r = pl.ds(pl.multiple_of(c_me * 32, 32), 32)
    mine_c = pl.ds(pl.multiple_of(r_me * 32, 32), 32)
    extra = [
        pltpu.make_async_copy(req_ref.at[mine_r], small.at[0], in_sem.at[2]),
        pltpu.make_async_copy(obj_ref.at[mine_c], small.at[1], in_sem.at[2]),
        pltpu.make_async_copy(low_ref.at[mine_c], small.at[2], in_sem.at[2]),
        pltpu.make_async_copy(up_ref.at[mine_c], small.at[3], in_sem.at[2]),
        pltpu.make_async_copy(ckind_ref.at[mine_r], ismall.at[0], in_sem.at[3]),
        pltpu.make_async_copy(vkind_ref.at[mine_c], ismall.at[1], in_sem.at[3]),
    ]
    for cp in extra:
        cp.start()

    whole(tab, in_sem.at[4])
    tables[2].wait()
    lane = lax.broadcasted_iota(jnp.int32, (8, 128), 1)
    count = count_ref[0, 0]
    ridx = jnp.full((8, 128), -1, jnp.int32)
    cidx = jnp.full((8, 128), -1, jnp.int32)
    for t in range(SLOTS):
        here = (lax.rem(lane, SLOTS) == t) & (lane < 2 * SLOTS) & (jnp.full((8, 128), t, jnp.int32) < count)
        ridx = jnp.where(here, tab[0, 0, t], ridx)
        cidx = jnp.where(here, tab[1, 0, t], cidx)
    p_iota = lax.broadcasted_iota(jnp.int32, (ROW_BLOCKS, 128), 0)
    r_iota = ((p_iota // 8 % 8) * 2 + p_iota // 64) * 8 + p_iota % 8
    c_iota = lax.broadcasted_iota(jnp.int32, (COL_BLOCKS, 128), 0)
    r_hot = jnp.where(r_iota == ridx[:1], 1.0, 0.0).astype(BF16)[:, : 2 * SLOTS]
    c_hot = jnp.where(c_iota == cidx[:1], 1.0, 0.0).astype(BF16)[:, : 2 * SLOTS]

    pl.semaphore_wait(barrier, len(near))

    def send(src, dst, phase, recv, dev):
        cp = pltpu.make_async_remote_copy(
            src_ref=src,
            dst_ref=dst,
            send_sem=sent_sem.at[phase],
            recv_sem=recv if not isinstance(recv, str) else recv_sem.at[RECV.index(recv)],
            device_id=dev,
            device_id_type=MESH_ID,
        )
        cp.start()
        return cp

    def arrived(ref, name):
        whole(ref, recv_sem.at[RECV.index(name)])

    def place(g, at, recv, dev):
        send(g.at[pl.ds(at * 8, 8)], g.at[pl.ds(at * 8, 8)], 0, recv, dev)

    place(yg, c_me, "y_n", y_near)
    place(xg, r_me, "x_far", y_far)
    place(yg, c_me, "y_x2", x_dev(2))
    for d in (2, 1, 3):
        place(xg, r_me, "x_z", z_dev(d))
    for d in (1, 3):
        place(yg, c_me, "y_x", x_dev(d))
    place(yg, c_me, "y_d", other)

    def convert(*which):
        for t in which:
            for g, (begin, _) in enumerate(BATCHES):
                if t == begin:
                    tile_copy(g).wait()
            for i in range(BLK // 128):
                sl = slice(i * 128, i * 128 + 128)
                v = tiles[t, sl, :]
                if t in VECTOR:
                    turned[VECTOR.index(t), :, sl] = v.T
                else:
                    m = MATRIX.index(t)
                    a_hi[m, sl, :], a_lo[m, sl, :] = split2(v)
                    t_hi[m, :, sl], t_lo[m, :, sl] = split2(v.T)

    convert(*range(6))
    arrived(yg.at[pl.ds(0, 8)], "y_n")
    at = ((1 - yl) * 4 + x) * 2 + core
    for c in (core, 1 - core):
        for d in (1, 3):
            place(yg, at, "y_d", (z, yh, yl, up4(x, d), c))
    place(yg, at, "y_d", other)
    convert(6, 7)
    arrived(yg.at[pl.ds(0, 8)], "y_x2")
    at = (yl * 4 + up4(x, 2)) * 2 + core
    for c in (core, 1 - core):
        place(yg, at, "y_d", (z, yh, 1 - yl, x, c))
    place(yg, at, "y_d", other)
    convert(8, 9)
    arrived(xg.at[pl.ds(0, 8)], "x_far")
    for d in (2, 1, 3):
        place(xg, z * 2 + 1 - yh, "x_z", z_dev(d))
    convert(10, 11)
    arrived(yg.at[pl.ds(0, 16)], "y_x")
    for d in (1, 3):
        place(yg, (yl * 4 + up4(x, d)) * 2 + core, "y_d", other)
    convert(*range(12, SLOTS))

    def scatter(hot, dest, blocks, base, rows):
        cols = []
        for e in rows:
            v = pbuf[pl.ds(e, SLOTS, stride=8), :]
            cols.append(jnp.concatenate(split2(v), axis=0))
        rhs = jnp.concatenate(cols, axis=1)
        out = jnp.dot(hot, rhs, preferred_element_type=F32)
        for i in range(len(rows)):
            dest[pl.ds(base + i, blocks, stride=len(rows)), :] = out[:, i * 128 : (i + 1) * 128]

    sub = lax.broadcasted_iota(jnp.int32, (8, 128), 0)

    def vector_product(v, at, groups):
        out = jnp.zeros((8, 128), F32)
        for g in groups:
            sums = [None, None]
            for k in range(4):
                block = at(slice(g * 128, g * 128 + 128), slice(k * 128, k * 128 + 128))
                for s in range(2):
                    term = block * v[2 * k + s : 2 * k + s + 1, :]
                    sums[s] = term if sums[s] is None else sums[s] + term
            for s in range(2):
                out = jnp.where(sub == 2 * g + s, jnp.sum(sums[s].T, axis=0, keepdims=True), out)
        return out

    def products(vec, index, hi_ref, lo_ref, plain_ref, plain, groups):
        lanes = slice(groups[0] * 128, groups[-1] * 128 + 128)
        rows = slice(2 * groups[0], 2 * groups[-1] + 2)
        for t in range(SLOTS):
            v = vec[tab[index, 0, t]]
            if t in VECTOR:
                n = plain.index(t)
                out = vector_product(v, lambda r, c, n=n: plain_ref[n, r, c], groups)
            else:
                m = MATRIX.index(t)
                lhs = spread(v)
                res = jnp.dot(lhs, hi_ref[m, :, lanes], preferred_element_type=F32)
                res = res + jnp.dot(lhs, lo_ref[m, :, lanes], preferred_element_type=F32)
                out = gathered(res, groups)
            pbuf[8 * t + rows.start : 8 * t + rows.stop, :] = out[rows]

    def own_rows(zz, hh):
        return pl.ds(pl.multiple_of((zz * 2 + hh) * OWN, OWN), OWN)

    def half_rows(h, c, chip, chips=1):
        return pl.ds(pl.multiple_of(h * HALF + (c * 8 + chip) * 32, 32), chips * 32)

    arrived(yg.at[pl.ds(0, 88)], "y_d")
    products(yg, 0, a_hi, a_lo, turned, VECTOR, range(4))
    scatter(c_hot, tpart, COL_BLOCKS, 0, range(8))
    for w, hh in enumerate((1 - yh, yh)):
        for i, d in enumerate((2, 1, 3)):
            send(tpart.at[own_rows(up4(z, d), hh)], zrecv.at[w, i], 1, ("z_far", "z_near")[w], z_dev(d))
    arrived(xg.at[pl.ds(0, 48)], "x_z")
    for h in range(2):
        products(xg, 1, t_hi, t_lo, tiles, list(range(SLOTS)), range(2 * h, 2 * h + 2))
        scatter(r_hot, part, ROW_BLOCKS, h * HALF, range(4 * h, 4 * h + 4))
        send(part.at[half_rows(h, 1 - core, 0, 8)], drecv.at[h], 1, ("d_0", "d_1")[h], other)
    def hand_out(h, steps):
        for i, off in enumerate(CHIP_OFFS[:-1]):
            if off[0] in steps:
                ny, nx = lax.rem(yl + off[0], 2), up4(x, off[1])
                dev = (z, yh, ny, nx, core)
                send(part.at[half_rows(h, core, ny * 4 + nx)], precv.at[i, pl.ds(32 * h, 32)], 1, "p_rs", dev)

    for h in range(2):
        arrived(drecv.at[h], ("d_0", "d_1")[h])
        mine = half_rows(h, core, 0, 8)
        part[mine, :] = part[mine, :] + drecv[h]
        hand_out(h, (0, 1) if h == 0 else (0,))
    arrived(zrecv.at[0], "z_far")
    zsum[...] = tpart[own_rows(z, 1 - yh), :] + zrecv[0, 0] + zrecv[0, 1] + zrecv[0, 2]
    send(zsum, yrecv, 1, "y_rs", y_far)
    hand_out(1, (1,))
    whole(small, in_sem.at[2])
    whole(ismall, in_sem.at[3])
    arrived(zrecv.at[1], "z_near")
    near_sum = tpart[own_rows(z, yh), :] + zrecv[1, 0] + zrecv[1, 1] + zrecv[1, 2]
    dual_own = [yg.reshape(ROW_BLOCKS * 8, 128)[pl.ds(c_me * OWN + s, 32, stride=2), :] for s in range(2)]
    primal_own = [xg.reshape(COL_BLOCKS * 8, 128)[pl.ds(r_me * OWN + s, 32, stride=2), :] for s in range(2)]
    stat_rows = [[], []]

    def total(v):
        return jnp.sum(v.reshape(4, 8, 128), axis=0)

    lane1 = lax.broadcasted_iota(jnp.int32, (1, 128), 1)

    def lane_sums(acc, begin, end):
        for s in range(2):
            for q in range(begin, end):
                v = jnp.sum(stat_rows[s][q], axis=0, keepdims=True)
                v = jnp.sum(v, axis=1, keepdims=True)
                acc = jnp.where(lane1 == 7 * s + q, v, acc)
        return acc

    arrived(yrecv, "y_rs")
    dres_ref[...] = near_sum + yrecv[...]
    obj, low, up, vk = small[1], small[2], small[3], ismall[1]
    low_on = (vk == 1) | (vk == 3)
    up_on = (vk == 2) | (vk == 3)
    for s in range(2):
        reduced = obj - dres_ref[pl.ds(s, 32, stride=2), :]
        mult = jnp.where(low_on, jnp.maximum(reduced, 0.0), 0.0) + jnp.where(
            up_on, jnp.minimum(reduced, 0.0), 0.0
        )
        res = reduced - mult
        dres_ref[pl.ds(s, 32, stride=2), :] = res
        bound = low * jnp.maximum(mult, 0.0) + up * jnp.minimum(mult, 0.0)
        stat_rows[s] += [
            total(res * res),
            total(obj * obj),
            total(obj * primal_own[s]),
            total(bound),
        ]
    acc = lane_sums(jnp.zeros((1, 128), F32), 0, 4)
    arrived(precv, "p_rs")
    for h in range(2):
        product = part[half_rows(h, core, yl * 4 + x), :]
        for i in range(7):
            product = product + precv[i, 32 * h : 32 * h + 32, :]
        psum[32 * h : 32 * h + 32, :] = product
    for h in range(2):
        for e in range(4):
            pres_ref[pl.ds(4 * h + e, 8, stride=8), :] = psum[pl.ds(32 * h + e, 8, stride=4), :]
    req = small[0]
    is_ge = ismall[0] == 1
    for s in range(2):
        diff = req - pres_ref[pl.ds(s, 32, stride=2), :]
        res = jnp.where(is_ge, jnp.maximum(diff, 0.0), diff)
        pres_ref[pl.ds(s, 32, stride=2), :] = res
        stat_rows[s] += [total(res * res), total(req * req), total(req * dual_own[s])]

    me = r_me * 16 + c_me
    stats[me] = lane_sums(acc, 4, 7)
    for dz, dh, dl, dx, dc in PEERS:
        dev = (up4(z, dz), lax.rem(yh + dh, 2), lax.rem(yl + dl, 2), up4(x, dx), lax.rem(core + dc, 2))
        send(stats.at[me], stats.at[me], 2, "stat", dev)
    arrived(stats.at[pl.ds(0, 127)], "stat")
    acc = jnp.sum(stats[...], axis=0)

    pick = [jnp.concatenate([acc[:, q : q + 1], acc[:, 7 + q : 8 + q]], axis=0) for q in range(7)]
    primal_square, require_square, require_dot = pick[4], pick[5], pick[6]
    dual_square, objective_square, objective_dot, bound_sum = pick[0], pick[1], pick[2], pick[3]
    primal_ratio = jnp.sqrt(primal_square) / (1.0 + jnp.sqrt(require_square))
    dual_ratio = jnp.sqrt(dual_square) / (1.0 + jnp.sqrt(objective_square))
    dual_value = require_dot + bound_sum
    gap = jnp.abs(objective_dot - dual_value) / (1.0 + jnp.abs(objective_dot) + jnp.abs(dual_value))
    lane2 = lax.broadcasted_iota(jnp.int32, (2, 128), 1)
    met = jnp.where(lane2 == 0, primal_ratio, jnp.where(lane2 == 1, dual_ratio, gap))
    met_ref[...] = met[:, :3]

    whole(tiles.at[0, pl.ds(0, 352)], sent_sem.at[0])
    whole(tiles.at[0, pl.ds(0, 352)], sent_sem.at[1])
    whole(stats.at[pl.ds(0, 127)], sent_sem.at[2])


def flush(a, b, c, a_out, b_out, c_out, sem):
    copies = [
        pltpu.make_async_copy(src, dst, sem.at[i])
        for i, (src, dst) in enumerate(((a, a_out), (b, b_out), (c, c_out)))
    ]
    for cp in copies:
        cp.start()
    for cp in copies:
        cp.wait()


def interleave(a):
    return a.reshape(2, 32, 128).transpose(1, 0, 2).reshape(OWN, 128)


def deinterleave(a):
    return a.reshape(32, 2, 128).transpose(1, 0, 2).reshape(2, 4096)


def on_device(
    matrix_tiles,
    tile_rows,
    tile_columns,
    tile_counts,
    primal_iter,
    dual_iter,
    requirement,
    constraint_kind,
    objective,
    lower_bound,
    upper_bound,
    variable_kind,
):
    hbm = pl.BlockSpec(memory_space=pl.ANY)
    vmem = pl.BlockSpec(memory_space=pltpu.VMEM)
    dma = pltpu.SemaphoreType.DMA
    pres, dres, metrics = pl.pallas_call(
        kernel,
        name="restart_check",
        out_shape=(
            pltpu.VMEM((OWN, 128), F32),
            pltpu.VMEM((OWN, 128), F32),
            pltpu.VMEM((2, 3), F32),
        ),
        in_specs=[hbm] * 12,
        out_specs=(vmem, vmem, vmem),
        scratch_shapes=[
            pltpu.SMEM((2, 1, SLOTS), jnp.int32),
            pltpu.SMEM((1, 1), jnp.int32),
            pltpu.VMEM((SLOTS, BLK, BLK), F32),
            pltpu.VMEM((len(MATRIX), BLK, BLK), BF16),
            pltpu.VMEM((len(MATRIX), BLK, BLK), BF16),
            pltpu.VMEM((len(MATRIX), BLK, BLK), BF16),
            pltpu.VMEM((len(MATRIX), BLK, BLK), BF16),
            pltpu.VMEM((len(VECTOR), BLK, BLK), F32),
            pltpu.VMEM((COL_BLOCKS, 8, 128), F32),
            pltpu.VMEM((ROW_BLOCKS, 8, 128), F32),
            pltpu.VMEM((SLOTS * 8, 128), F32),
            pltpu.VMEM((16 * OWN, 128), F32),
            pltpu.VMEM((8 * OWN, 128), F32),
            pltpu.VMEM((2, HALF // 2, 128), F32),
            pltpu.VMEM((7, OWN, 128), F32),
            pltpu.VMEM((OWN, 128), F32),
            pltpu.VMEM((2, 3, OWN, 128), F32),
            pltpu.VMEM((OWN, 128), F32),
            pltpu.VMEM((OWN, 128), F32),
            pltpu.VMEM((4, 32, 128), F32),
            pltpu.VMEM((2, 32, 128), jnp.int32),
            pltpu.VMEM((128, 1, 128), F32),
            dma((len(BATCHES),)),
            dma((6,)),
            dma((3,)),
            dma((len(RECV),)),
        ],
        compiler_params=pltpu.CompilerParams(
            collective_id=0, has_side_effects=True, vmem_limit_bytes=60 * 1024 * 1024
        ),
    )(
        tile_rows.reshape(1, SLOTS),
        tile_columns.reshape(1, SLOTS),
        tile_counts,
        matrix_tiles.reshape(SLOTS, BLK, BLK),
        interleave(primal_iter),
        interleave(dual_iter),
        requirement.reshape(512, 128),
        constraint_kind.reshape(512, 128),
        objective.reshape(256, 128),
        lower_bound.reshape(256, 128),
        upper_bound.reshape(256, 128),
        variable_kind.reshape(256, 128),
    )
    pres, dres, metrics = pl.pallas_call(
        flush,
        name="flush",
        out_shape=(
            pltpu.HBM((OWN, 128), F32),
            pltpu.HBM((OWN, 128), F32),
            pltpu.HBM((2, 3), F32),
        ),
        in_specs=[vmem] * 3,
        out_specs=(hbm,) * 3,
        scratch_shapes=[dma((3,))],
        compiler_params=pltpu.CompilerParams(vmem_limit_bytes=1024 * 1024),
    )(pres, dres, metrics)
    return deinterleave(pres), deinterleave(dres), metrics


def solution(mesh):
    torus = Mesh(mesh.devices.reshape(4, 2, 2, 4, 2), ROW_COL)
    return jax.shard_map(
        on_device,
        mesh=torus,
        in_specs=(
            P(ROW, COL, None, None, None),
            P(ROW, COL, None),
            P(ROW, COL, None),
            P(ROW, COL),
            P(None, COL_ROW),
            P(None, ROW_COL),
            P(ROW),
            P(ROW),
            P(COL),
            P(COL),
            P(COL),
            P(COL),
        ),
        out_specs=(P(None, ROW_COL), P(None, COL_ROW), P()),
        check_vma=False,
    )
```
